64 devices in a mesh: dp: 4 (over x, y), sp: 16 (over z, core).
Axes of the slice: x: 2, y: 2, z: 8, core: 2. Of those that a mesh axis runs over, the one named last changes fastest.
The devices are a block of a 4x4x8 slice.
Arguments:
- x: bfloat16 [8192, 6144], P(('dp', 'sp')), parts along dimension 0
- gain: bfloat16 [6144], replicated
- wq: bfloat16 [6144, 6144], replicated
- wk: bfloat16 [6144, 1024], replicated
- wv: bfloat16 [6144, 1024], replicated
- wo: bfloat16 [6144, 6144], replicated
Outputs:
- output: bfloat16 [8192, 6144], P(('dp', 'sp')), parts along dimension 0
There are 4 independent parts. The reference program is written for one: setup_inputs(seed, part) draws one part's arguments, and reference() takes and returns one part's arrays. A program takes and returns all parts, laid end to end along the dimension named above; an argument that names none is the same for every part.
All inputs are finite; a program needn't handle non-finite values.
Results may differ from the reference program's by a relative error of at most 0.012.
Values are sent between devices in bfloat16 or wider.
A program may use at most 768 MiB of HBM per device.

```python
import jax
import jax.numpy as jnp
from jax import lax

ROWS = 2048
D = 6144
HEADS = 48
KV_HEADS = 8
HEAD = 128
THETA = 10000


def setup_inputs(seed: int = 0, part: int = 0) -> dict:
    kx, kn, kq, kk, kv, ko = jax.random.split(jax.random.key(seed), 6)

    def weights(key, rows, columns):
        return jax.random.normal(key, (rows, columns), jnp.float32) * rows**-0.5

    drawn = {
        "x": jax.random.normal(jax.random.fold_in(kx, part), (ROWS, D), jnp.float32),
        "gain": 1 + 0.1 * jax.random.normal(kn, (D,), jnp.float32),
        "wq": 2 * weights(kq, D, HEADS * HEAD),
        "wk": 2 * weights(kk, D, KV_HEADS * HEAD),
        "wv": 4 * weights(kv, D, KV_HEADS * HEAD),
        "wo": weights(ko, HEADS * HEAD, D),
    }
    return {k: v.astype(jnp.bfloat16) for k, v in drawn.items()}


def normed(x, gain):
    wide = x.astype(jnp.float32)
    scale = lax.rsqrt(jnp.mean(wide * wide, -1, keepdims=True) + 1e-6)
    return (wide * scale * gain.astype(jnp.float32)).astype(jnp.bfloat16)


def turned(t, place, theta):
    half = t.shape[-1] // 2
    angle = place.astype(jnp.float32)[:, None] * theta ** (-jnp.arange(half, dtype=jnp.float32) / half)
    cos, sin = jnp.cos(angle)[:, None], jnp.sin(angle)[:, None]
    a, b = t[..., :half].astype(jnp.float32), t[..., half:].astype(jnp.float32)
    return jnp.concatenate([a * cos - b * sin, b * cos + a * sin], -1).astype(jnp.bfloat16)


def matmul(a, w):
    return jnp.dot(a, w, preferred_element_type=jnp.float32).astype(jnp.bfloat16)


def einsum(form, a, b):
    return jnp.einsum(form, a.astype(jnp.float32), b.astype(jnp.float32))


def attention(q, k, v):
    scores = einsum("tgsd,ugd->gstu", q, k) * q.shape[-1] ** -0.5
    token = jnp.arange(q.shape[0])
    scores = jnp.where(token[:, None] >= token, scores, -jnp.inf)
    weights = jax.nn.softmax(scores, -1).astype(jnp.bfloat16)
    return einsum("gstu,ugd->tgsd", weights, v).astype(jnp.bfloat16)


def reference(x, gain, wq, wk, wv, wo):
    a, place = normed(x, gain), jnp.arange(ROWS)
    q = turned(matmul(a, wq).reshape(ROWS, HEADS, HEAD), place, THETA).reshape(ROWS, KV_HEADS, -1, HEAD)
    k = turned(matmul(a, wk).reshape(ROWS, KV_HEADS, HEAD), place, THETA)
    v = matmul(a, wv).reshape(ROWS, KV_HEADS, HEAD)
    seen = attention(q, k, v).reshape(ROWS, HEADS * HEAD)
    return (x.astype(jnp.float32) + jnp.dot(seen, wo, preferred_element_type=jnp.float32)).astype(jnp.bfloat16)
```

```python
import functools

import jax
import jax.numpy as jnp
from jax import lax
from jax.experimental import pallas as pl
from jax.experimental.pallas import tpu as pltpu
from jax.sharding import PartitionSpec as P

HEAD = 128
THETA = 10000
HIDDEN = -2e30
LOG2E = 1.4426950408889634
VMEM = 63 * 2**20
SLAB = 512
WIDE = 512
OUTW = 512
SLOTS = 5

bf16, f32 = jnp.bfloat16, jnp.float32


def _dot(a, b, ca, cb):
    return lax.dot_general(a, b, (((ca,), (cb,)), ((), ())), preferred_element_type=f32)


def _kernel(n, x_hbm, gain_ref, cos_ref, sin_ref, wq, wk, wv, wo, out_hbm,
            x_s, a_s, q_s, kv_s, stage_s, top_s, mix_s, seen_s, acc_s, slab_s, wo_s,
            x_sem, slab_sem, wo_sem, xs_send, xs_recv, s1_send, s1_recv, sp_recv, f_send, f_recv,
            seen_send, seen_recv, out_sem, y_send, y_recv):
    me = lax.axis_index("sp")
    c, z = lax.rem(me, 2), lax.div(me, 2)
    nz = n // 2
    partner = me + 1 - 2 * c
    left, right = lax.rem(z + nz - 1, nz), lax.rem(z + 1, nz)
    own, dim = x_hbm.shape
    both = 2 * own
    hk = kv_s.shape[0]
    g = q_s.shape[0] // (both * hk)
    cols = g * both
    kvw, qw = wk.shape[1] // 2, wq.shape[1] // 2
    yw = dim // 2
    pairs = hk // 2
    gw = g * HEAD
    e = HEAD**-0.5 * LOG2E

    def chunk_at(offset):
        return lax.rem(z + offset + 2 * nz, nz)

    def remote(src, dst, send, recv, to):
        return pltpu.make_async_remote_copy(src_ref=src, dst_ref=dst, send_sem=send, recv_sem=recv, device_id={"sp": to},
                                            device_id_type=pl.DeviceIdType.MESH)

    def slab_copies(step, slot):
        at = pl.multiple_of((c if step % 2 == 0 else 1 - c) * kvw + (step // 2) * 2 * HEAD, 2 * HEAD)
        return [pltpu.make_async_copy(w.at[:, pl.ds(at, SLAB // 2)], slab_s.at[slot, :, pl.ds(i * (SLAB // 2), SLAB // 2)],
                                      slab_sem.at[slot, i]) for i, w in enumerate((wk, wv))]

    def q_copies(i, slot):
        return [pltpu.make_async_copy(wq.at[:, pl.ds(pl.multiple_of(c * qw + i * SLAB + k * (SLAB // 2), SLAB // 2), SLAB // 2)],
                                      slab_s.at[slot, :, pl.ds(k * (SLAB // 2), SLAB // 2)], slab_sem.at[slot, k]) for k in range(2)]

    def wo_copies(t):
        slot, whose = t % SLOTS, (c if t % 2 == 0 else 1 - c)
        row = whose * qw + (t // 2) * gw
        half = gw // 2
        return [pltpu.make_async_copy(wo.at[pl.ds(pl.multiple_of(row + k * half, half), half), pl.ds(pl.multiple_of(c * yw, yw), yw)],
                                      wo_s.at[slot, pl.ds(k * half, half), :], wo_sem.at[slot, k]) for k in range(2)]

    mine = pl.ds(pl.multiple_of(c * own, own), own)
    theirs = pl.ds(pl.multiple_of((1 - c) * own, own), own)
    x_copy = pltpu.make_async_copy(x_hbm, x_s.at[mine, :], x_sem)
    x_copy.start()
    for step in range(2):
        for copy in slab_copies(step, step):
            copy.start()

    barrier = pltpu.get_barrier_semaphore()
    near = [partner, left * 2 + c, right * 2 + c, left * 2 + 1 - c, right * 2 + 1 - c]
    for to in near:
        pl.semaphore_signal(barrier, inc=1, device_id={"sp": to}, device_id_type=pl.DeviceIdType.MESH)
    pl.semaphore_wait(barrier, len(near))

    x_copy.wait()
    x_send = remote(x_s.at[mine, :], x_s.at[mine, :], xs_send, xs_recv, partner)
    x_send.start()

    def norm_rows(start):
        def rows(i, _):
            r = pl.ds(pl.multiple_of(start + i * 16, 16), 16)
            wide = x_s[r, :].astype(f32)
            scale = lax.rsqrt(jnp.mean(wide * wide, -1, keepdims=True) + 1e-6)
            a_s[r, :] = (wide * scale * gain_ref[...].astype(f32)).astype(bf16)

        lax.fori_loop(0, own // 16, rows, None)

    norm_rows(c * own)

    def turned(t, cos, sin):
        t = t.astype(bf16).astype(f32)
        return (t * cos + pltpu.roll(t, HEAD // 2, 1) * sin).astype(bf16)

    first_sends = []
    for step in range(2 * pairs):
        slot, p, other = step % 2, step // 2, step % 2
        for copy in slab_copies(step, slot):
            copy.wait()
        made = _dot(a_s[mine, :], slab_s[slot], 1, 0)
        if step + 2 < 2 * pairs:
            for copy in slab_copies(step + 2, slot):
                copy.start()
        else:
            for copy in q_copies(step + 2 - 2 * pairs, slot):
                copy.start()
        cos, sin = cos_ref[mine, :], sin_ref[mine, :]
        for i in range(2):
            k = turned(made[:, i * HEAD : (i + 1) * HEAD], cos, sin)
            v = made[:, (2 + i) * HEAD : (3 + i) * HEAD].T.astype(bf16)
            if other:
                stage_s[p, i, 0], stage_s[p, i, 1] = k, v
            else:
                kv_s[2 * p + i, 0, me], kv_s[2 * p + i, 1, me] = k, v
        dst = kv_s.at[pl.ds(2 * p, 2), :, me]
        src = stage_s.at[p] if other else dst
        core = 1 - c if other else c
        sends = [remote(src, dst, s1_send.at[step, 0], s1_recv.at[0, other, p], right * 2 + core),
                 remote(src, dst, s1_send.at[step, 1], s1_recv.at[1, other, p], left * 2 + core)]
        if other:
            sends.append(remote(src, dst, s1_send.at[step, 2], sp_recv.at[p], partner))
        for copy in sends:
            copy.start()
        first_sends += sends

    x_send.wait_send()
    remote(x_s.at[theirs, :], x_s.at[theirs, :], xs_send, xs_recv, partner).wait_recv()
    norm_rows((1 - c) * own)

    def part(d, s, h, at):
        blocks = pl.ds(pl.multiple_of(2 * at, 2), 2)
        return kv_s.at[h, :, blocks] if s < nz // 2 else kv_s.at[h, d, blocks]

    def passing(d, s, h):
        at = chunk_at(-(s - 1) if d == 0 else s - 1)
        ref = part(d, s, h, at)
        return remote(ref, ref, f_send.at[d, s - 2, h], f_recv.at[d, s - 2, h], (right if d == 0 else left) * 2 + c)

    def coming(d, s, h):
        ref = part(d, s, h, chunk_at(-s if d == 0 else s))
        return remote(ref, ref, f_send.at[d, s - 2, h], f_recv.at[d, s - 2, h], partner)

    def first_arrived(p):
        for d in range(2):
            for other in range(2):
                block = chunk_at(-1 if d == 0 else 1) * 2 + (1 - c if other else c)
                ref = kv_s.at[pl.ds(2 * p, 2), :, block]
                remote(ref, ref, xs_send, s1_recv.at[d, other, p], partner).wait_recv()

    def forward(s, h, wait=True):
        for d in range(2):
            if wait:
                coming(d, s - 1, h).wait_recv()
            passing(d, s, h).start()

    def q_step(i, _):
        slot = lax.rem(i, 2)
        for copy in q_copies(i, slot):
            copy.wait()
        made = _dot(a_s[...], slab_s[slot], 1, 0)

        @pl.when(i < qw // SLAB - 2)
        def _():
            for copy in q_copies(i + 2, slot):
                copy.start()

        cos, sin = cos_ref[...], sin_ref[...]
        for k in range(SLAB // HEAD):
            at = pl.multiple_of((i * (SLAB // HEAD) + k) * both, both)
            q_s[pl.ds(at, both), :] = turned(made[:, k * HEAD : (k + 1) * HEAD], cos, sin)

        for p in range(pairs):
            @pl.when(i == 2 * p + 1)
            def _():
                first_arrived(p)
                for h in (2 * p, 2 * p + 1):
                    forward(2, h, wait=False)

    lax.fori_loop(0, qw // SLAB, q_step, None)
    forward(3, 0)
    for t in range(SLOTS):
        for copy in wo_copies(t):
            copy.start()
    for p in range(pairs):
        ref = kv_s.at[pl.ds(2 * p, 2), :, me + 1 - 2 * c]
        remote(ref, ref, xs_send, sp_recv.at[p], partner).wait_recv()

    ats = list(range(0, cols, WIDE))

    def attend(h, chunks, own_chunk=False):
        keys = jnp.concatenate([kv_s[h, 0, pl.ds(2 * b, 2)].reshape(both, HEAD) for b in chunks], axis=0)
        values = jnp.concatenate([kv_s[h, 1, 2 * b + i] for b in chunks for i in range(2)], axis=1)
        values = jnp.concatenate([values, jnp.ones((8, values.shape[1]), bf16)], axis=0)
        scores = [_dot(keys, q_s[pl.ds(pl.multiple_of(h * cols + at, WIDE), WIDE), :], 1, 1) for at in ats]
        if own_chunk:
            shape = (both, WIDE)
            ok = lax.broadcasted_iota(jnp.int32, shape, 0) <= lax.rem(lax.broadcasted_iota(jnp.int32, shape, 1), both)
        weights, keeps = [], []
        for at, s in zip(ats, scores):
            if own_chunk:
                s = jnp.where(ok, s, HIDDEN)
                top = s.max(axis=0, keepdims=True)
            else:
                old = top_s[h, :, at : at + WIDE]
                top = jnp.maximum(old, s.max(axis=0, keepdims=True))
                keeps.append(jnp.exp2((old - top) * e))
            top_s[h, :, at : at + WIDE] = top
            weights.append(jnp.exp2((s - top) * e).astype(bf16))
        for i, (at, w) in enumerate(zip(ats, weights)):
            add = _dot(values, w, 1, 0)
            mix_s[h, :, at : at + WIDE] = add if own_chunk else mix_s[h, :, at : at + WIDE] * keeps[i] + add

    def attend_at(h, s):
        before, after = z >= s, z + s >= nz
        lower, upper = chunk_at(-s), chunk_at(s)
        if 2 * s == nz:
            @pl.when(before)
            def _():
                attend(h, [lower])
        else:
            @pl.when(before & after)
            def _():
                attend(h, [lower, upper])

            @pl.when(before != after)
            def _():
                attend(h, [jnp.where(before, lower, upper)])

    def own_stage(h, _):
        attend(h, [z], own_chunk=True)

        @pl.when(h == 1)
        def _():
            forward(3, 1)

    lax.fori_loop(0, hk, own_stage, None)

    def stage_1(h, _):
        attend_at(h, 1)

        @pl.when(lax.rem(h, 2) == 1)
        def _():
            forward(3, 2 + lax.div(h, 2))

    lax.fori_loop(0, hk, stage_1, None)

    def stage_2(h, _):
        attend_at(h, 2)

        @pl.when(lax.rem(h, 2) == 1)
        def _():
            forward(4, lax.div(h, 2))

    lax.fori_loop(0, hk, stage_2, None)

    def project(t, init=False, last=False):
        grp, whose, slot = t // 2, (c if t % 2 == 0 else 1 - c), t % SLOTS
        if t % 2 == 1:
            ref = seen_s.at[1 - c, grp]
            remote(ref, ref, seen_send.at[grp], seen_recv.at[grp], partner).wait_recv()
        for copy in wo_copies(t):
            copy.wait()

        def block(i, _):
            at = pl.ds(pl.multiple_of(i * OUTW, OUTW), OUTW)
            add = _dot(seen_s[whose, grp], wo_s[slot, :, at], 1, 0)
            if init:
                acc_s[:, at] = x_s[:, pl.ds(pl.multiple_of(c * yw + i * OUTW, OUTW), OUTW)].astype(f32) + add
            elif last:
                a_s[:, at] = (acc_s[:, at] + add).astype(bf16)
                for copy in out_copies(i):
                    copy.start()
            else:
                acc_s[:, at] = acc_s[:, at] + add

        lax.fori_loop(0, yw // OUTW, block, None)
        if t + SLOTS < 2 * hk:
            for copy in wo_copies(t + SLOTS):
                copy.start()

    def out_copies(i):
        at = pl.ds(pl.multiple_of(i * OUTW, OUTW), OUTW)
        to = pl.ds(pl.multiple_of(c * yw + i * OUTW, OUTW), OUTW)
        return [remote(a_s.at[theirs, at], out_hbm.at[:, to], y_send.at[i], y_recv.at[i], partner),
                pltpu.make_async_copy(a_s.at[mine, at], out_hbm.at[:, to], out_sem.at[i])]

    def seen_copy(h):
        ref = seen_s.at[c, h]
        return remote(ref, ref, seen_send.at[h], seen_recv.at[h], partner)

    def tail(h):
        attend_at(h, 3)
        for d in range(2):
            coming(d, 4, h).wait_recv()
        attend_at(h, 4)
        inverse = 1 / mix_s[h, HEAD : HEAD + 1, :]
        for k in range(g):
            at = slice(k * both, (k + 1) * both)
            seen_s[c, h, :, k * HEAD : (k + 1) * HEAD] = (mix_s[h, :HEAD, at] * inverse[:, at]).T.astype(bf16)
        seen_copy(h).start()
        if h:
            project(2 * h - 2, init=h == 1)
            project(2 * h - 1)
        if h < 2:
            forward(4, h + 2)

    for h in range(hk):
        tail(h)
    project(2 * hk - 2)
    project(2 * hk - 1, last=True)

    for copy in first_sends:
        copy.wait_send()
    for s in (2, 3, 4):
        for h in range(hk):
            for d in range(2):
                passing(d, s, h).wait_send()
    for h in range(hk):
        seen_copy(h).wait_send()
    for i in range(yw // OUTW):
        sent, kept = out_copies(i)
        sent.wait_send()
        kept.wait()
        to = pl.ds(pl.multiple_of((1 - c) * yw + i * OUTW, OUTW), OUTW)
        remote(out_hbm.at[:, to], out_hbm.at[:, to], y_send.at[i], y_recv.at[i], partner).wait_recv()


def solution(mesh):
    n = mesh.shape["sp"]

    def step(x, gain, wq, wk, wv, wo):
        own, dim = x.shape
        both = 2 * own
        hk = wk.shape[1] // HEAD // 2
        qw = wq.shape[1] // 2
        g = qw // HEAD // hk
        cols = g * both
        place = (lax.axis_index("sp") // 2) * both + jnp.arange(both)
        half = HEAD // 2
        angle = place.astype(f32)[:, None] * THETA ** (-jnp.arange(half, dtype=f32) / half)
        cos, sin = jnp.cos(angle), jnp.sin(angle)
        cos, sin = jnp.concatenate([cos, cos], -1), jnp.concatenate([-sin, sin], -1)
        vmem, hbm = pl.BlockSpec(memory_space=pltpu.VMEM), pl.BlockSpec(memory_space=pl.ANY)
        dma = pltpu.SemaphoreType.DMA
        blocks = dim // 2 // OUTW
        return pl.pallas_call(
            functools.partial(_kernel, n),
            out_shape=jax.ShapeDtypeStruct((own, dim), bf16),
            in_specs=[hbm, vmem, vmem, vmem, hbm, hbm, hbm, hbm],
            out_specs=hbm,
            scratch_shapes=[
                pltpu.VMEM((both, dim), bf16),
                pltpu.VMEM((both, dim), bf16),
                pltpu.VMEM((hk * g * both, HEAD), bf16),
                pltpu.VMEM((hk, 2, n, own, HEAD), bf16),
                pltpu.VMEM((hk // 2, 2, 2, own, HEAD), bf16),
                pltpu.VMEM((hk, 1, cols), f32),
                pltpu.VMEM((hk, HEAD + 8, cols), f32),
                pltpu.VMEM((2, hk, both, g * HEAD), bf16),
                pltpu.VMEM((both, dim // 2), f32),
                pltpu.VMEM((2, dim, SLAB), bf16),
                pltpu.VMEM((SLOTS, g * HEAD, dim // 2), bf16),
                dma, dma((2, 2)), dma((SLOTS, 2)), dma, dma, dma((hk, 3)), dma((2, 2, hk // 2)), dma((hk // 2,)),
                dma((2, 3, hk)), dma((2, 3, hk)), dma((hk,)), dma((hk,)), dma((blocks,)), dma((blocks,)), dma((blocks,)),
            ],
            compiler_params=pltpu.CompilerParams(collective_id=0, has_side_effects=True, vmem_limit_bytes=VMEM),
        )(x, gain.reshape(1, dim), cos, sin, wq, wk, wv, wo)

    tokens, whole = P(("dp", "sp"), None), P(None, None)
    return jax.shard_map(
        step,
        mesh=mesh,
        in_specs=(tokens, P(None), whole, whole, whole, whole),
        out_specs=tokens,
        check_vma=False,
    )
```

```python
import functools
import math

import jax
import jax.numpy as jnp
from jax import lax
from jax.experimental import pallas as pl
from jax.experimental.pallas import tpu as pltpu
from jax.sharding import PartitionSpec as P

HEAD = 128
THETA = 10000
HIDDEN = -2e30
LOG2E = 1.4426950408889634
VMEM = 63 * 2**20
SLAB = 512
WIDE = 512
OUTW = 1024
SLABS = 3
ROWS = 16

bf16, f32 = jnp.bfloat16, jnp.float32


def _dot(a, b, ca, cb):
    return lax.dot_general(a, b, (((ca,), (cb,)), ((), ())), preferred_element_type=f32)


def _kernel(n, x_hbm, gain_ref, wq, wk, wv, wo, out_hbm, gain_s, cos_ref, sin_ref, x_s, a_s, q_s, kv_s, stage_s, made_s, top_s, mix_s, seen_s, acc_s, slab_s, wo_s,
            x_sem, slab_sem, wo_sem, xs_send, xs_recv, s1_send, s1_recv, sp_recv, f_send, f_recv,
            seen_send, seen_recv, out_sem, y_send, y_recv):
    me = lax.axis_index("sp")
    c, z = lax.rem(me, 2), lax.div(me, 2)
    nz = n // 2
    partner = me + 1 - 2 * c
    left, right = lax.rem(z + nz - 1, nz), lax.rem(z + 1, nz)
    own, dim = x_hbm.shape
    both = 2 * own
    hk = kv_s.shape[0]
    g = q_s.shape[0] // (both * hk)
    cols = g * both
    kvw, qw = wk.shape[1] // 2, wq.shape[1] // 2
    yw = dim // 2
    pairs = hk // 2
    gw = g * HEAD
    e = HEAD**-0.5 * LOG2E

    def chunk_at(offset):
        return lax.rem(z + offset + 2 * nz, nz)

    def wanted(d, s, to):
        return to >= s if d == 0 else (to + s >= nz) | (to + s < nz // 2)

    def remote(src, dst, send, recv, to):
        return pltpu.make_async_remote_copy(src_ref=src, dst_ref=dst, send_sem=send, recv_sem=recv, device_id={"sp": to},
                                            device_id_type=pl.DeviceIdType.MESH)

    def slab_copies(step, slot):
        at = pl.multiple_of((c if step % 2 == 0 else 1 - c) * kvw + (step // 2) * 2 * HEAD, 2 * HEAD)
        return [pltpu.make_async_copy(w.at[:, pl.ds(at, SLAB // 2)], slab_s.at[slot, :, pl.ds(i * (SLAB // 2), SLAB // 2)],
                                      slab_sem.at[slot, i]) for i, w in enumerate((wk, wv))]

    def q_copies(i, slot):
        return [pltpu.make_async_copy(wq.at[:, pl.ds(pl.multiple_of(c * qw + i * SLAB + k * (SLAB // 2), SLAB // 2), SLAB // 2)],
                                      slab_s.at[slot, :, pl.ds(k * (SLAB // 2), SLAB // 2)], slab_sem.at[slot, k]) for k in range(2)]

    def wo_copies(grp, k):
        row = (1 - c if k else c) * qw + grp * gw
        half = gw // 2
        return [pltpu.make_async_copy(wo.at[pl.ds(pl.multiple_of(row + i * half, half), half), pl.ds(pl.multiple_of(c * yw, yw), yw)],
                                      wo_s.at[lax.rem(grp, 2), k, pl.ds(i * half, half), :], wo_sem.at[lax.rem(grp, 2), k, i])
                for i in range(2)]

    mine = pl.ds(pl.multiple_of(c * own, own), own)
    theirs = pl.ds(pl.multiple_of((1 - c) * own, own), own)
    x_copy = pltpu.make_async_copy(x_hbm, x_s.at[mine, :], x_sem)
    x_copy.start()
    for copy in slab_copies(0, 0):
        copy.start()

    barrier = pltpu.get_barrier_semaphore()
    near = [partner, left * 2 + c, right * 2 + c, left * 2 + 1 - c, right * 2 + 1 - c]
    for to in near:
        pl.semaphore_signal(barrier, inc=1, device_id={"sp": to}, device_id_type=pl.DeviceIdType.MESH)

    for i in range(dim // HEAD):
        gain_s[:, i * HEAD : (i + 1) * HEAD] = jnp.broadcast_to(gain_ref[i : i + 1, :].astype(f32), (ROWS, HEAD))
    element = lax.broadcasted_iota(jnp.int32, (both, HEAD), 1)
    half = HEAD // 2
    power = jnp.where(element < half, element, element - half).astype(f32)
    place = (z * both + lax.broadcasted_iota(jnp.int32, (both, HEAD), 0)).astype(f32)
    angle = place * jnp.exp2(power * (-math.log2(THETA) / half))
    cos_ref[...] = jnp.cos(angle)
    sine = jnp.sin(angle)
    sin_ref[...] = jnp.where(element < half, -sine, sine)

    x_copy.wait()
    for copy in slab_copies(1, 1):
        copy.start()

    def norm_rows(start):
        def rows(i, _):
            for k in range(2):
                r = pl.ds(pl.multiple_of(start + (2 * i + k) * ROWS, ROWS), ROWS)
                wide = x_s[r, :].astype(f32)
                scale = lax.rsqrt(jnp.mean(wide * wide, -1, keepdims=True) + 1e-6)
                a_s[r, :] = (wide * scale * gain_s[...]).astype(bf16)

        lax.fori_loop(0, own // ROWS // 2, rows, None)

    norm_rows(c * own)
    pl.semaphore_wait(barrier, len(near))
    x_send = remote(x_s.at[mine, :], x_s.at[mine, :], xs_send, xs_recv, partner)
    x_send.start()

    def turned(t, cos, sin):
        t = t.astype(bf16).astype(f32)
        return (t * cos + pltpu.roll(t, HEAD // 2, 1) * sin).astype(bf16)

    first_sends = []
    for step in range(2 * pairs):
        slot, p, other = step % SLABS, step // 2, step % 2
        if step == 0:
            for copy in slab_copies(2, 2):
                copy.start()
        for copy in slab_copies(step, slot):
            copy.wait()
        made = _dot(a_s[mine, :], slab_s[slot], 1, 0)
        if step + SLABS < 2 * pairs:
            for copy in slab_copies(step + SLABS, slot):
                copy.start()
        else:
            for copy in q_copies(step + SLABS - 2 * pairs, slot):
                copy.start()
        cos, sin = cos_ref[mine, :], sin_ref[mine, :]
        for i in range(2):
            k = turned(made[:, i * HEAD : (i + 1) * HEAD], cos, sin)
            v = made[:, (2 + i) * HEAD : (3 + i) * HEAD].T.astype(bf16)
            if other:
                stage_s[p, i, 0], stage_s[p, i, 1] = k, v
            else:
                kv_s[2 * p + i, 0, me], kv_s[2 * p + i, 1, me] = k, v
        dst = kv_s.at[pl.ds(2 * p, 2), :, me]
        src = stage_s.at[p] if other else dst
        core = 1 - c if other else c
        sends = [(wanted(0, 1, right), remote(src, dst, s1_send.at[step, 0], s1_recv.at[0, other, p], right * 2 + core)),
                 (wanted(1, 1, left), remote(src, dst, s1_send.at[step, 1], s1_recv.at[1, other, p], left * 2 + core))]
        if other:
            sends.append((True, remote(src, dst, s1_send.at[step, 2], sp_recv.at[p], partner)))
        for needed, copy in sends:
            pl.when(needed)(copy.start)
        first_sends += sends
        if step == 1:
            x_send.wait_send()
            remote(x_s.at[theirs, :], x_s.at[theirs, :], xs_send, xs_recv, partner).wait_recv()
            norm_rows((1 - c) * own)

    def part(d, s, h, at):
        blocks = pl.ds(pl.multiple_of(2 * at, 2), 2)
        return kv_s.at[h, :, blocks] if s < nz // 2 else kv_s.at[h, d, blocks]

    def passing(d, s, h):
        at = chunk_at(-(s - 1) if d == 0 else s - 1)
        ref = part(d, s, h, at)
        return remote(ref, ref, f_send.at[d, s - 2, h], f_recv.at[d, s - 2, h], (right if d == 0 else left) * 2 + c)

    def coming(d, s, h):
        ref = part(d, s, h, chunk_at(-s if d == 0 else s))
        return remote(ref, ref, f_send.at[d, s - 2, h], f_recv.at[d, s - 2, h], partner)

    def first_arrived(p):
        for d in range(2):
            @pl.when(wanted(d, 1, z))
            def _():
                for other in range(2):
                    block = chunk_at(-1 if d == 0 else 1) * 2 + (1 - c if other else c)
                    ref = kv_s.at[pl.ds(2 * p, 2), :, block]
                    remote(ref, ref, xs_send, s1_recv.at[d, other, p], partner).wait_recv()

    def arrived(s, h):
        for d in range(2):
            pl.when(wanted(d, s, z))(coming(d, s, h).wait_recv)

    def forward(s, h):
        for d in range(2):
            pl.when(wanted(d, s, right if d == 0 else left))(passing(d, s, h).start)

    def turn_queries(i):
        for k in range(SLAB // HEAD):
            at = pl.multiple_of((i * (SLAB // HEAD) + k) * both, both)
            q_s[pl.ds(at, both), :] = turned(made_s[:, k * HEAD : (k + 1) * HEAD], cos_ref[...], sin_ref[...])

    made_s[...] = jnp.zeros((both, SLAB), f32)

    def q_step(i, _):
        slot = lax.rem(i + 2 * pairs, SLABS)
        for copy in q_copies(i, slot):
            copy.wait()
        turn_queries(jnp.maximum(i - 1, 0))
        made_s[...] = _dot(a_s[...], slab_s[slot], 1, 0)
        at = pl.ds(pl.multiple_of(i * SLAB, SLAB), SLAB)
        acc_s[:, at] = x_s[:, pl.ds(pl.multiple_of(c * yw + i * SLAB, SLAB), SLAB)].astype(f32)

        @pl.when(i < qw // SLAB - SLABS)
        def _():
            for copy in q_copies(i + SLABS, slot):
                copy.start()

        @pl.when(i == 1)
        def _():
            first_arrived(0)
            forward(2, 0)
            forward(2, 1)

        @pl.when(i == 4)
        def _():
            arrived(2, 0)
            forward(3, 0)
            first_arrived(1)
            forward(2, 2)

    lax.fori_loop(0, qw // SLAB, q_step, None)
    turn_queries(qw // SLAB - 1)
    for grp in range(2):
        for k in range(2):
            for copy in wo_copies(grp, k):
                copy.start()
    for p in range(pairs):
        ref = kv_s.at[pl.ds(2 * p, 2), :, me + 1 - 2 * c]
        remote(ref, ref, xs_send, sp_recv.at[p], partner).wait_recv()

    def attend(p, heads, chunks, own_chunk=False):
        strips = [(i, at) for i in heads for at in range(0, cols, WIDE)]
        loaded = {}
        if own_chunk:
            shape = (both, WIDE)
            ok = lax.broadcasted_iota(jnp.int32, shape, 0) <= lax.rem(lax.broadcasted_iota(jnp.int32, shape, 1), both)

        def keys_of(i):
            if i not in loaded:
                h = 2 * p + i
                keys = jnp.concatenate([kv_s[h, 0, pl.ds(2 * b, 2)].reshape(both, HEAD) for b in chunks], axis=0)
                values = jnp.concatenate([kv_s[h, 1, 2 * b + j] for b in chunks for j in range(2)], axis=1)
                loaded[i] = keys, jnp.concatenate([values, jnp.ones((8, values.shape[1]), bf16)], axis=0)
            return loaded[i]

        def score(i, at):
            return _dot(keys_of(i)[0], q_s[pl.ds(pl.multiple_of((2 * p + i) * cols + at, WIDE), WIDE), :], 1, 1)

        scores = [score(*strip) for strip in strips[:2]]
        for m, (i, at) in enumerate(strips):
            if m + 2 < len(strips):
                scores.append(score(*strips[m + 2]))
            s, here = scores[m], slice(at, at + WIDE)
            if own_chunk:
                s = jnp.where(ok, s, HIDDEN)
                top = s.max(axis=0, keepdims=True)
            else:
                old = top_s[p, i, :, here]
                top = jnp.maximum(old, s.max(axis=0, keepdims=True))
            top_s[p, i, :, here] = top
            add = _dot(keys_of(i)[1], jnp.exp2((s - top) * e).astype(bf16), 1, 0)
            mix_s[p, i, :, here] = add if own_chunk else mix_s[p, i, :, here] * jnp.exp2((old - top) * e) + add

    def attend_at(p, s):
        before, after = z >= s, z + s >= nz
        lower, upper = chunk_at(-s), chunk_at(s)

        @pl.when(before & after)
        def _():
            attend(p, (0, 1), [lower, upper])

        @pl.when(before != after)
        def _():
            attend(p, (0, 1), [jnp.where(before, lower, upper)])

    def seen_copy(h):
        ref = seen_s.at[c, h]
        return remote(ref, ref, seen_send.at[h], seen_recv.at[h], partner)

    def seen_arrived(h):
        ref = seen_s.at[1 - c, h]
        remote(ref, ref, seen_send.at[h], seen_recv.at[h], partner).wait_recv()

    def product(grp, k, at):
        return _dot(seen_s[1 - c if k else c, grp], wo_s[lax.rem(grp, 2), k, :, at], 1, 0)

    def blocks(body):
        def block(i, _):
            body(i, pl.ds(pl.multiple_of(i * OUTW, OUTW), OUTW))

        lax.fori_loop(0, yw // OUTW, block, None)

    def project(grp):
        seen_arrived(grp)
        for k in range(2):
            for copy in wo_copies(grp, k):
                copy.wait()

        def body(_, at):
            acc_s[:, at] = acc_s[:, at] + (product(grp, 0, at) + product(grp, 1, at))

        blocks(body)

        @pl.when(grp + 2 < hk)
        def _():
            for k in range(2):
                for copy in wo_copies(grp + 2, k):
                    copy.start()

    def out_copies(i):
        at = pl.ds(pl.multiple_of(i * OUTW, OUTW), OUTW)
        to = pl.ds(pl.multiple_of(c * yw + i * OUTW, OUTW), OUTW)
        return [remote(a_s.at[theirs, at], out_hbm.at[:, to], y_send.at[i], y_recv.at[i], partner),
                pltpu.make_async_copy(a_s.at[mine, at], out_hbm.at[:, to], out_sem.at[i])]

    def finish(h, p, i):
        arrived(nz // 2, h)

        @pl.when(z >= nz // 2)
        def _():
            attend(p, (i,), [chunk_at(nz // 2)])

        inverse = 1 / mix_s[p, i, HEAD : HEAD + 1, :]
        for k in range(g):
            at = slice(k * both, (k + 1) * both)
            seen_s[c, h, :, k * HEAD : (k + 1) * HEAD] = (mix_s[p, i, :HEAD, at] * inverse[:, at]).T.astype(bf16)
        seen_copy(h).start()

    order = [(0, 0), (0, 1), (0, 2), (1, 0), (1, 1), (0, 3), (1, 2), (1, 3)]

    def pick(k, values):
        at = jnp.int32(values[-1])
        for n_, value in enumerate(values[:-1]):
            at = jnp.where(k == n_, value, at)
        return at

    def stage(k, _):
        p, s = pick(k, [a for a, _ in order]), pick(k, [b for _, b in order])

        @pl.when(s == 0)
        def _():
            attend(p, (0, 1), [z], own_chunk=True)

        @pl.when(s > 0)
        def _():
            attend_at(p, s)

        @pl.when(k == 0)
        def _():
            arrived(2, 1)
            forward(3, 1)

        @pl.when(k == 2)
        def _():
            arrived(3, 0)
            forward(4, 0)
            forward(2, 3)

        @pl.when(k == 4)
        def _():
            arrived(3, 1)
            forward(4, 1)
            arrived(2, 2)
            forward(3, 2)

        @pl.when(k == 5)
        def _():
            finish(0, 0, 0)
            arrived(2, 3)
            forward(3, 3)
            project(0)
            finish(1, 0, 1)

        @pl.when(k == 6)
        def _():
            arrived(3, 2)
            forward(4, 2)
            project(1)
            arrived(3, 3)
            forward(4, 3)

    lax.fori_loop(0, len(order), stage, None)
    finish(2, 1, 0)
    project(2)
    finish(3, 1, 1)

    last = hk - 1
    for copy in wo_copies(last, 0):
        copy.wait()

    def own_part(_, at):
        acc_s[:, at] = acc_s[:, at] + product(last, 0, at)

    blocks(own_part)
    for copy in wo_copies(last, 1):
        copy.wait()
    seen_arrived(last)

    def final_part(i, at):
        a_s[:, at] = (acc_s[:, at] + product(last, 1, at)).astype(bf16)
        for copy in out_copies(i):
            copy.start()

    blocks(final_part)

    for needed, copy in first_sends:
        pl.when(needed)(copy.wait_send)
    for d in range(2):
        for s in range(2, nz // 2 + 1):
            @pl.when(wanted(d, s, right if d == 0 else left))
            def _():
                for h in range(hk):
                    passing(d, s, h).wait_send()
    for h in range(hk):
        seen_copy(h).wait_send()
    for i in range(yw // OUTW):
        sent, kept = out_copies(i)
        sent.wait_send()
        kept.wait()
        to = pl.ds(pl.multiple_of((1 - c) * yw + i * OUTW, OUTW), OUTW)
        remote(out_hbm.at[:, to], out_hbm.at[:, to], y_send.at[i], y_recv.at[i], partner).wait_recv()


def solution(mesh):
    n = mesh.shape["sp"]

    def step(x, gain, wq, wk, wv, wo):
        own, dim = x.shape
        both = 2 * own
        hk = wk.shape[1] // HEAD // 2
        qw = wq.shape[1] // 2
        g = qw // HEAD // hk
        cols = g * both
        vmem, hbm = pl.BlockSpec(memory_space=pltpu.VMEM), pl.BlockSpec(memory_space=pl.ANY)
        dma = pltpu.SemaphoreType.DMA
        blocks = dim // 2 // OUTW
        return pl.pallas_call(
            functools.partial(_kernel, n),
            out_shape=jax.ShapeDtypeStruct((own, dim), bf16),
            in_specs=[hbm, vmem, hbm, hbm, hbm, hbm],
            out_specs=hbm,
            scratch_shapes=[
                pltpu.VMEM((ROWS, dim), f32),
                pltpu.VMEM((both, HEAD), f32),
                pltpu.VMEM((both, HEAD), f32),
                pltpu.VMEM((both, dim), bf16),
                pltpu.VMEM((both, dim), bf16),
                pltpu.VMEM((hk * g * both, HEAD), bf16),
                pltpu.VMEM((hk, 2, n, own, HEAD), bf16),
                pltpu.VMEM((hk // 2, 2, 2, own, HEAD), bf16),
                pltpu.VMEM((both, SLAB), f32),
                pltpu.VMEM((hk // 2, 2, 1, cols), f32),
                pltpu.VMEM((hk // 2, 2, HEAD + 8, cols), f32),
                pltpu.VMEM((2, hk, both, g * HEAD), bf16),
                pltpu.VMEM((both, dim // 2), f32),
                pltpu.VMEM((SLABS, dim, SLAB), bf16),
                pltpu.VMEM((2, 2, g * HEAD, dim // 2), bf16),
                dma, dma((SLABS, 2)), dma((2, 2, 2)), dma, dma, dma((hk, 3)), dma((2, 2, hk // 2)), dma((hk // 2,)),
                dma((2, 3, hk)), dma((2, 3, hk)), dma((hk,)), dma((hk,)), dma((blocks,)), dma((blocks,)), dma((blocks,)),
            ],
            compiler_params=pltpu.CompilerParams(collective_id=0, has_side_effects=True, vmem_limit_bytes=VMEM),
        )(x, gain.reshape(dim // HEAD, HEAD), wq, wk, wv, wo)

    tokens, whole = P(("dp", "sp"), None), P(None, None)
    return jax.shard_map(
        step,
        mesh=mesh,
        in_specs=(tokens, P(None), whole, whole, whole, whole),
        out_specs=tokens,
        check_vma=False,
    )
```

```python
import functools
import math

import jax
import jax.numpy as jnp
from jax import lax
from jax.experimental import pallas as pl
from jax.experimental.pallas import tpu as pltpu
from jax.sharding import PartitionSpec as P

HEAD = 128
THETA = 10000
HIDDEN = -2e30
LOG2E = 1.4426950408889634
VMEM = 62 * 2**20
SLAB = 512
WIDE = 256
AHEAD = 3
OUTW = 1536
LASTW = 1024
SLABS = 3
ROWS = 16

bf16, f32 = jnp.bfloat16, jnp.float32


def _dot(a, b, ca, cb):
    return lax.dot_general(a, b, (((ca,), (cb,)), ((), ())), preferred_element_type=f32)


def _kernel(n, x_hbm, gain_ref, wq, wk, wv, wo, out_ref, gain_s, cos_ref, sin_ref, x_s, a_s, q_s, kv_s, stage_s, made_s, top_s, mix_s, acc_s, slab_s, wo_s,
            x_sem, slab_sem, wo_sem, xs_send, xs_recv, s1_send, s1_recv, sp_recv, f_send, f_recv,
            seen_send, seen_recv, y_send, y_recv, ready):
    me = lax.axis_index("sp")
    c, z = lax.rem(me, 2), lax.div(me, 2)
    nz = n // 2
    partner = me + 1 - 2 * c
    left, right = lax.rem(z + nz - 1, nz), lax.rem(z + 1, nz)
    own, dim = x_hbm.shape
    both = 2 * own
    hk = kv_s.shape[0]
    g = q_s.shape[0] // (both * hk)
    cols = g * both
    kvw, qw = wk.shape[1] // 2, wq.shape[1] // 2
    yw = dim // 2
    pairs = hk // 2
    kv_steps = pairs + 1
    gw = g * HEAD
    e = HEAD**-0.5 * LOG2E

    def chunk_at(offset):
        return lax.rem(z + offset + 2 * nz, nz)

    def wanted(d, s, to):
        return to >= s if d == 0 else (to + s >= nz) | (to + s < nz // 2)

    def remote(src, dst, send, recv, to):
        return pltpu.make_async_remote_copy(src_ref=src, dst_ref=dst, send_sem=send, recv_sem=recv, device_id={"sp": to},
                                            device_id_type=pl.DeviceIdType.MESH)

    def slab_copies(step, slot):
        at = pl.multiple_of((1 - c if step == 1 else c) * kvw + max(step - 1, 0) * 2 * HEAD, 2 * HEAD)
        return [pltpu.make_async_copy(w.at[:, pl.ds(at, SLAB // 2)], slab_s.at[slot, :, pl.ds(i * (SLAB // 2), SLAB // 2)],
                                      slab_sem.at[slot, i]) for i, w in enumerate((wk, wv))]

    def q_copies(i, slot):
        return [pltpu.make_async_copy(wq.at[:, pl.ds(pl.multiple_of(c * qw + i * SLAB + k * (SLAB // 2), SLAB // 2), SLAB // 2)],
                                      slab_s.at[slot, :, pl.ds(k * (SLAB // 2), SLAB // 2)], slab_sem.at[slot, k]) for k in range(2)]

    def wo_copies(grp, k):
        row = (1 - c if k else c) * qw + grp * gw
        half = gw // 2
        return [pltpu.make_async_copy(wo.at[pl.ds(pl.multiple_of(row + i * half, half), half), pl.ds(pl.multiple_of(c * yw, yw), yw)],
                                      wo_s.at[grp % 2, k, pl.ds(i * half, half), :], wo_sem.at[grp % 2, k, i])
                for i in range(2)]

    mine = pl.ds(pl.multiple_of(c * own, own), own)
    theirs = pl.ds(pl.multiple_of((1 - c) * own, own), own)
    x_copy = pltpu.make_async_copy(x_hbm, x_s.at[mine, :], x_sem)
    x_copy.start()
    slab_copies(0, 0)[0].start()

    barrier = pltpu.get_barrier_semaphore()
    near = [partner, left * 2 + c, right * 2 + c, left * 2 + 1 - c, right * 2 + 1 - c]
    for to in near:
        pl.semaphore_signal(barrier, inc=1, device_id={"sp": to}, device_id_type=pl.DeviceIdType.MESH)

    for i in range(dim // HEAD):
        gain_s[:, i * HEAD : (i + 1) * HEAD] = jnp.broadcast_to(gain_ref[i : i + 1, :].astype(f32), (ROWS, HEAD))
    element = lax.broadcasted_iota(jnp.int32, (both, HEAD), 1)
    half = HEAD // 2
    power = jnp.where(element < half, element, element - half).astype(f32)
    place = (z * both + lax.broadcasted_iota(jnp.int32, (both, HEAD), 0)).astype(f32)
    angle = place * jnp.exp2(power * (-math.log2(THETA) / half))
    cos_ref[...] = jnp.cos(angle)
    sine = jnp.sin(angle)
    sin_ref[...] = jnp.where(element < half, -sine, sine)

    x_copy.wait()
    slab_copies(0, 0)[1].start()
    for copy in slab_copies(1, 1):
        copy.start()

    def norm_rows(start):
        def rows(i, _):
            for k in range(2):
                r = pl.ds(pl.multiple_of(start + (2 * i + k) * ROWS, ROWS), ROWS)
                wide = x_s[r, :].astype(f32)
                scale = lax.rsqrt(jnp.mean(wide * wide, -1, keepdims=True) + 1e-6)
                a_s[r, :] = (wide * scale * gain_s[...]).astype(bf16)

        lax.fori_loop(0, own // ROWS // 2, rows, None)

    norm_rows(c * own)
    pl.semaphore_wait(barrier, len(near))
    x_send = remote(x_s.at[mine, :], x_s.at[mine, :], xs_send, xs_recv, partner)
    x_send.start()

    def turned(t, cos, sin):
        t = t.astype(bf16).astype(f32)
        return (t * cos + pltpu.roll(t, HEAD // 2, 1) * sin).astype(bf16)

    first_sends = []
    for step in range(kv_steps):
        slot, p, other = step % SLABS, max(step - 1, 0), step == 1
        pooled = step > 1
        if step == 0:
            for copy in slab_copies(2, 2):
                copy.start()
        for copy in slab_copies(step, slot):
            copy.wait()
        made = _dot(a_s[...] if pooled else a_s[mine, :], slab_s[slot], 1, 0)
        if step + SLABS < kv_steps:
            for copy in slab_copies(step + SLABS, slot):
                copy.start()
        else:
            for copy in q_copies(step + SLABS - kv_steps, slot):
                copy.start()
        cos, sin = (cos_ref[...], sin_ref[...]) if pooled else (cos_ref[mine, :], sin_ref[mine, :])
        for i in range(2):
            k = turned(made[:, i * HEAD : (i + 1) * HEAD], cos, sin)
            v = made[:, (2 + i) * HEAD : (3 + i) * HEAD].T.astype(bf16)
            if other:
                stage_s[i, 0], stage_s[i, 1] = k, v
            elif pooled:
                for j in range(2):
                    kv_s[2 * p + i, 0, 2 * z + j] = k[j * own : (j + 1) * own, :]
                    kv_s[2 * p + i, 1, 2 * z + j] = v[:, j * own : (j + 1) * own]
            else:
                kv_s[2 * p + i, 0, me], kv_s[2 * p + i, 1, me] = k, v
        dst = kv_s.at[pl.ds(2 * p, 2), :, pl.ds(pl.multiple_of(2 * z, 2), 2) if pooled else me]
        src = stage_s if other else dst
        core = 1 - c if other else c
        sends = [(wanted(0, 1, right), remote(src, dst, s1_send.at[step, 0], s1_recv.at[0, step], right * 2 + core)),
                 (wanted(1, 1, left), remote(src, dst, s1_send.at[step, 1], s1_recv.at[1, step], left * 2 + core))]
        if other:
            sends.append((True, remote(src, dst, s1_send.at[step, 2], sp_recv, partner)))
        for needed, copy in sends:
            pl.when(needed)(copy.start)
        first_sends += sends
        if step == 1:
            x_send.wait_send()
            remote(x_s.at[theirs, :], x_s.at[theirs, :], xs_send, xs_recv, partner).wait_recv()
            norm_rows((1 - c) * own)

    def part(d, s, h, at):
        blocks = pl.ds(pl.multiple_of(2 * at, 2), 2)
        return kv_s.at[h, :, blocks] if s < nz // 2 else kv_s.at[h, d, blocks]

    def passing(d, s, h):
        at = chunk_at(-(s - 1) if d == 0 else s - 1)
        ref = part(d, s, h, at)
        return remote(ref, ref, f_send.at[d, s - 2, h], f_recv.at[d, s - 2, h], (right if d == 0 else left) * 2 + c)

    def coming(d, s, h):
        ref = part(d, s, h, chunk_at(-s if d == 0 else s))
        return remote(ref, ref, f_send.at[d, s - 2, h], f_recv.at[d, s - 2, h], partner)

    def first_arrived(p):
        for d in range(2):
            @pl.when(wanted(d, 1, z))
            def _():
                at = chunk_at(-1 if d == 0 else 1)
                if p == 0:
                    whose = [(0, at * 2 + c), (1, at * 2 + 1 - c)]
                else:
                    whose = [(p + 1, pl.ds(pl.multiple_of(2 * at, 2), 2))]
                for step, block in whose:
                    ref = kv_s.at[pl.ds(2 * p, 2), :, block]
                    remote(ref, ref, xs_send, s1_recv.at[d, step], partner).wait_recv()

    def arrived(s, h):
        for d in range(2):
            pl.when(wanted(d, s, z))(coming(d, s, h).wait_recv)

    def forward(s, h):
        for d in range(2):
            pl.when(wanted(d, s, right if d == 0 else left))(passing(d, s, h).start)

    def turn_queries(i):
        for k in range(SLAB // HEAD):
            at = pl.multiple_of((i * (SLAB // HEAD) + k) * both, both)
            q_s[pl.ds(at, both), :] = turned(made_s[:, k * HEAD : (k + 1) * HEAD], cos_ref[...], sin_ref[...])

    made_s[...] = jnp.zeros((both, SLAB), f32)

    def q_step(i, _):
        slot = lax.rem(i + kv_steps, SLABS)
        for copy in q_copies(i, slot):
            copy.wait()
        turn_queries(jnp.maximum(i - 1, 0))
        made_s[...] = _dot(a_s[...], slab_s[slot], 1, 0)
        at = pl.ds(pl.multiple_of(i * SLAB, SLAB), SLAB)
        acc_s[:, at] = x_s[:, pl.ds(pl.multiple_of(c * yw + i * SLAB, SLAB), SLAB)].astype(f32)

        @pl.when(i < qw // SLAB - SLABS)
        def _():
            for copy in q_copies(i + SLABS, slot):
                copy.start()

        @pl.when(i == 2)
        def _():
            first_arrived(0)
            forward(2, 0)
            forward(2, 1)

    lax.fori_loop(0, qw // SLAB, q_step, None)
    pl.semaphore_signal(ready, inc=1, device_id={"sp": partner}, device_id_type=pl.DeviceIdType.MESH)
    turn_queries(qw // SLAB - 1)
    for grp in range(2):
        for k in range(2):
            for copy in wo_copies(grp, k):
                copy.start()
    ref = kv_s.at[pl.ds(0, 2), :, partner]
    remote(ref, ref, xs_send, sp_recv, partner).wait_recv()

    def attend(p, heads, chunks, own_chunk=False):
        strips = [(i, at) for i in heads for at in range(0, cols, WIDE)]
        loaded = {}
        if own_chunk:
            shape = (both, WIDE)
            ok = lax.broadcasted_iota(jnp.int32, shape, 0) <= lax.rem(lax.broadcasted_iota(jnp.int32, shape, 1), both)

        def keys_of(i):
            if i not in loaded:
                h = 2 * p + i
                keys = jnp.concatenate([kv_s[h, 0, pl.ds(2 * b, 2)].reshape(both, HEAD) for b in chunks], axis=0)
                values = jnp.concatenate([kv_s[h, 1, 2 * b + j] for b in chunks for j in range(2)], axis=1)
                loaded[i] = keys, jnp.concatenate([values, jnp.ones((8, values.shape[1]), bf16)], axis=0)
            return loaded[i]

        def score(i, at):
            return _dot(keys_of(i)[0], q_s[pl.ds(pl.multiple_of((2 * p + i) * cols + at, WIDE), WIDE), :], 1, 1) * e

        scores = [score(*strip) for strip in strips[:AHEAD]]
        for m, (i, at) in enumerate(strips):
            if m + AHEAD < len(strips):
                scores.append(score(*strips[m + AHEAD]))
            s, here = scores[m], slice(at, at + WIDE)
            if own_chunk:
                s = jnp.where(ok, s, HIDDEN)
                top = s.max(axis=0, keepdims=True)
            else:
                old = top_s[p, i, :, here]
                top = jnp.maximum(old, s.max(axis=0, keepdims=True))
            top_s[p, i, :, here] = top
            add = _dot(keys_of(i)[1], jnp.exp2(s - top).astype(bf16), 1, 0)
            mix_s[p, i, :, here] = add if own_chunk else mix_s[p, i, :, here] * jnp.exp2(old - top) + add

    def attend_at(p, s):
        before, after = z >= s, z + s >= nz
        lower, upper = chunk_at(-s), chunk_at(s)

        @pl.when(before & after)
        def _():
            attend(p, (0, 1), [lower, upper])

        @pl.when(before != after)
        def _():
            attend(p, (0, 1), [jnp.where(before, lower, upper)])

    def seen(whose, h):
        return x_s.at[:, pl.ds(pl.multiple_of(whose * qw + h * gw, gw), gw)]

    def seen_copy(h):
        return remote(seen(c, h), seen(c, h), seen_send.at[h], seen_recv.at[h], partner)

    def seen_arrived(h):
        remote(seen(1 - c, h), seen(1 - c, h), seen_send.at[h], seen_recv.at[h], partner).wait_recv()

    def product(grp, k, at):
        return _dot(seen(1 - c if k else c, grp)[...], wo_s[grp % 2, k, :, at], 1, 0)

    def blocks(body, width=OUTW):
        def block(i, _):
            body(i, pl.ds(pl.multiple_of(i * width, width), width))

        lax.fori_loop(0, yw // width, block, None)

    def project(grp, parts=(0, 1)):
        for k in parts:
            for copy in wo_copies(grp, k):
                copy.wait()
        if 1 in parts:
            seen_arrived(grp)

        def body(_, at):
            acc_s[:, at] = acc_s[:, at] + sum(product(grp, k, at) for k in parts)

        blocks(body)
        if 1 in parts and grp + 2 < hk:
            for k in range(2):
                for copy in wo_copies(grp + 2, k):
                    copy.start()

    def out_copy(i):
        at = pl.ds(pl.multiple_of(i * LASTW, LASTW), LASTW)
        to = pl.ds(pl.multiple_of(c * yw + i * LASTW, LASTW), LASTW)
        return remote(a_s.at[theirs, at], out_ref.at[:, to], y_send.at[i], y_recv.at[i], partner)

    def finish(h, p, i):
        arrived(nz // 2, h)

        @pl.when(z >= nz // 2)
        def _():
            attend(p, (i,), [chunk_at(nz // 2)])

        inverse = 1 / mix_s[p, i, HEAD : HEAD + 1, :]
        for k in range(g):
            at = slice(k * both, (k + 1) * both)
            seen(c, h)[:, k * HEAD : (k + 1) * HEAD] = (mix_s[p, i, :HEAD, at] * inverse[:, at]).T.astype(bf16)
        seen_copy(h).start()

    order = [(0, 0), (0, 1), (1, 0), (1, 1), (0, 2), (0, 3), (1, 2), (1, 3)]

    def pick(k, values):
        at = jnp.int32(values[-1])
        for n_, value in enumerate(values[:-1]):
            at = jnp.where(k == n_, value, at)
        return at

    def stage(k, _):
        p, s = pick(k, [a for a, _ in order]), pick(k, [b for _, b in order])

        @pl.when(s == 0)
        def _():
            attend(p, (0, 1), [z], own_chunk=True)

        @pl.when(s > 0)
        def _():
            attend_at(p, s)

        @pl.when(k == 0)
        def _():
            arrived(2, 0)
            forward(3, 0)

        @pl.when(k == 1)
        def _():
            arrived(2, 1)
            forward(3, 1)

        @pl.when(k == 2)
        def _():
            first_arrived(1)

        @pl.when(k == 3)
        def _():
            arrived(3, 0)
            forward(4, 0)
            forward(2, 2)

        @pl.when(k == 4)
        def _():
            arrived(3, 1)
            forward(4, 1)
            forward(2, 3)

        @pl.when(k == 5)
        def _():
            pl.semaphore_wait(ready, 1)
            finish(0, 0, 0)
            project(0, (0,))
            arrived(2, 2)
            forward(3, 2)
            finish(1, 0, 1)
            arrived(2, 3)
            forward(3, 3)
            project(0, (1,))

        @pl.when(k == 6)
        def _():
            arrived(3, 2)
            forward(4, 2)
            project(1)
            arrived(3, 3)
            forward(4, 3)

    lax.fori_loop(0, len(order), stage, None)
    finish(2, 1, 0)
    project(2, (0,))
    finish(3, 1, 1)
    project(2, (1,))

    last = hk - 1
    for k in range(2):
        for copy in wo_copies(last, k):
            copy.wait()
    seen_arrived(last)

    def final(i, at):
        a_s[:, at] = (acc_s[:, at] + (product(last, 0, at) + product(last, 1, at))).astype(bf16)
        out_copy(i).start()
        out_ref[:, pl.ds(pl.multiple_of(c * yw + i * LASTW, LASTW), LASTW)] = a_s[mine, at]

    blocks(final, LASTW)

    for needed, copy in first_sends:
        pl.when(needed)(copy.wait_send)
    for d in range(2):
        for s in range(2, nz // 2 + 1):
            @pl.when(wanted(d, s, right if d == 0 else left))
            def _():
                for h in range(hk):
                    passing(d, s, h).wait_send()
    for h in range(hk):
        seen_copy(h).wait_send()
    for i in range(yw // LASTW):
        out_copy(i).wait_send()
        to = pl.ds(pl.multiple_of((1 - c) * yw + i * LASTW, LASTW), LASTW)
        remote(out_ref.at[:, to], out_ref.at[:, to], y_send.at[i], y_recv.at[i], partner).wait_recv()


def solution(mesh):
    n = mesh.shape["sp"]

    def step(x, gain, wq, wk, wv, wo):
        own, dim = x.shape
        both = 2 * own
        hk = wk.shape[1] // HEAD // 2
        qw = wq.shape[1] // 2
        g = qw // HEAD // hk
        cols = g * both
        vmem, hbm = pl.BlockSpec(memory_space=pltpu.VMEM), pl.BlockSpec(memory_space=pl.ANY)
        dma = pltpu.SemaphoreType.DMA
        blocks = dim // 2 // LASTW
        return pl.pallas_call(
            functools.partial(_kernel, n),
            out_shape=pltpu.VMEM((own, dim), bf16),
            in_specs=[hbm, vmem, hbm, hbm, hbm, hbm],
            out_specs=vmem,
            scratch_shapes=[
                pltpu.VMEM((ROWS, dim), f32),
                pltpu.VMEM((both, HEAD), f32),
                pltpu.VMEM((both, HEAD), f32),
                pltpu.VMEM((both, dim), bf16),
                pltpu.VMEM((both, dim), bf16),
                pltpu.VMEM((hk * g * both, HEAD), bf16),
                pltpu.VMEM((hk, 2, n, own, HEAD), bf16),
                pltpu.VMEM((2, 2, own, HEAD), bf16),
                pltpu.VMEM((both, SLAB), f32),
                pltpu.VMEM((hk // 2, 2, 1, cols), f32),
                pltpu.VMEM((hk // 2, 2, HEAD + 8, cols), f32),
                pltpu.VMEM((both, dim // 2), f32),
                pltpu.VMEM((SLABS, dim, SLAB), bf16),
                pltpu.VMEM((2, 2, g * HEAD, dim // 2), bf16),
                dma, dma((SLABS, 2)), dma((2, 2, 2)), dma, dma, dma((hk // 2 + 1, 3)), dma((2, hk // 2 + 1)), dma,
                dma((2, 3, hk)), dma((2, 3, hk)), dma((hk,)), dma((hk,)), dma((blocks,)), dma((blocks,)), pltpu.SemaphoreType.REGULAR,
            ],
            compiler_params=pltpu.CompilerParams(collective_id=0, has_side_effects=True, vmem_limit_bytes=VMEM),
        )(x, gain.reshape(dim // HEAD, HEAD), wq, wk, wv, wo)

    tokens, whole = P(("dp", "sp"), None), P(None, None)
    return jax.shard_map(
        step,
        mesh=mesh,
        in_specs=(tokens, P(None), whole, whole, whole, whole),
        out_specs=tokens,
        check_vma=False,
    )
```

```python
import functools
import math

import jax
import jax.numpy as jnp
from jax import lax
from jax.experimental import pallas as pl
from jax.experimental.pallas import tpu as pltpu
from jax.sharding import PartitionSpec as P

HEAD = 128
THETA = 10000
HIDDEN = -2e30
LOG2E = 1.4426950408889634
VMEM = 62 * 2**20
SLAB = 512
WIDE = 256
AHEAD = 3
OUTW = 1536
LASTW = 1024
SLABS = 3
ROWS = 16

bf16, f32 = jnp.bfloat16, jnp.float32


def _dot(a, b, ca, cb):
    return lax.dot_general(a, b, (((ca,), (cb,)), ((), ())), preferred_element_type=f32)


def _kernel(n, x_hbm, gain_ref, wq, wk, wv, wo, out_ref, gain_s, cos_ref, sin_ref, x_s, a_s, q_s, kv_s, stage_s, made_s, top_s, mix_s, acc_s, slab_s, wo_s,
            x_sem, slab_sem, wo_sem, xs_send, xs_recv, s1_send, s1_recv, sp_recv, f_send, f_recv,
            seen_send, seen_recv, y_send, y_recv, ready):
    me = lax.axis_index("sp")
    c, z = lax.rem(me, 2), lax.div(me, 2)
    nz = n // 2
    partner = me + 1 - 2 * c
    left, right = lax.rem(z + nz - 1, nz), lax.rem(z + 1, nz)
    own, dim = x_hbm.shape
    both = 2 * own
    hk = kv_s.shape[0]
    g = q_s.shape[0] // (both * hk)
    cols = g * both
    kvw, qw = wk.shape[1] // 2, wq.shape[1] // 2
    yw = dim // 2
    pairs = hk // 2
    kv_steps = pairs + 1
    gw = g * HEAD
    e = HEAD**-0.5 * LOG2E

    def chunk_at(offset):
        return lax.rem(z + offset + 2 * nz, nz)

    def wanted(d, s, to):
        return to >= s if d == 0 else (to + s >= nz) | (to + s < nz // 2)

    def remote(src, dst, send, recv, to):
        return pltpu.make_async_remote_copy(src_ref=src, dst_ref=dst, send_sem=send, recv_sem=recv, device_id={"sp": to},
                                            device_id_type=pl.DeviceIdType.MESH)

    def slab_copies(step, slot):
        at = pl.multiple_of((1 - c if step == 1 else c) * kvw + max(step - 1, 0) * 2 * HEAD, 2 * HEAD)
        return [pltpu.make_async_copy(w.at[:, pl.ds(at, SLAB // 2)], slab_s.at[slot, :, pl.ds(i * (SLAB // 2), SLAB // 2)],
                                      slab_sem.at[slot, i]) for i, w in enumerate((wk, wv))]

    def q_copies(i, slot):
        return [pltpu.make_async_copy(wq.at[:, pl.ds(pl.multiple_of(c * qw + i * SLAB + k * (SLAB // 2), SLAB // 2), SLAB // 2)],
                                      slab_s.at[slot, :, pl.ds(k * (SLAB // 2), SLAB // 2)], slab_sem.at[slot, k]) for k in range(2)]

    def wo_copies(grp, k):
        row = (1 - c if k else c) * qw + grp * gw
        half = gw // 2
        return [pltpu.make_async_copy(wo.at[pl.ds(pl.multiple_of(row + i * half, half), half), pl.ds(pl.multiple_of(c * yw, yw), yw)],
                                      wo_s.at[grp % 2, k, pl.ds(i * half, half), :], wo_sem.at[grp % 2, k, i])
                for i in range(2)]

    mine = pl.ds(pl.multiple_of(c * own, own), own)
    theirs = pl.ds(pl.multiple_of((1 - c) * own, own), own)
    def fetch(step, k):
        (slab_copies(step, step % SLABS) if step < kv_steps else q_copies(step - kv_steps, step % SLABS))[k].start()

    x_copy = pltpu.make_async_copy(x_hbm, x_s.at[mine, :], x_sem)
    x_copy.start()
    fetch(0, 0)

    barrier = pltpu.get_barrier_semaphore()
    near = [partner, left * 2 + c, right * 2 + c, left * 2 + 1 - c, right * 2 + 1 - c]
    for to in near:
        pl.semaphore_signal(barrier, inc=1, device_id={"sp": to}, device_id_type=pl.DeviceIdType.MESH)

    for i in range(dim // HEAD):
        gain_s[:, i * HEAD : (i + 1) * HEAD] = jnp.broadcast_to(gain_ref[i : i + 1, :].astype(f32), (ROWS, HEAD))
    element = lax.broadcasted_iota(jnp.int32, (both, HEAD), 1)
    half = HEAD // 2
    power = jnp.where(element < half, element, element - half).astype(f32)
    place = (z * both + lax.broadcasted_iota(jnp.int32, (both, HEAD), 0)).astype(f32)
    angle = place * jnp.exp2(power * (-math.log2(THETA) / half))
    cos_ref[...] = jnp.cos(angle)
    sine = jnp.sin(angle)
    sin_ref[...] = jnp.where(element < half, -sine, sine)

    x_copy.wait()
    for step, k in ((0, 1), (1, 0), (1, 1)):
        fetch(step, k)

    def norm_rows(start):
        def rows(i, _):
            for k in range(2):
                r = pl.ds(pl.multiple_of(start + (2 * i + k) * ROWS, ROWS), ROWS)
                wide = x_s[r, :].astype(f32)
                scale = lax.rsqrt(jnp.mean(wide * wide, -1, keepdims=True) + 1e-6)
                a_s[r, :] = (wide * scale * gain_s[...]).astype(bf16)

        lax.fori_loop(0, own // ROWS // 2, rows, None)

    pl.semaphore_wait(barrier, len(near))
    x_send = remote(x_s.at[mine, :], x_s.at[mine, :], xs_send, xs_recv, partner)
    x_send.start()
    norm_rows(c * own)

    def turned(t, cos, sin):
        t = t.astype(bf16).astype(f32)
        return (t * cos + pltpu.roll(t, HEAD // 2, 1) * sin).astype(bf16)

    first_sends = []
    for step in range(kv_steps):
        slot, p, other = step % SLABS, max(step - 1, 0), step == 1
        pooled = step > 1
        tokens = slice(None) if pooled else mine
        core = 1 - c if other else c
        block = pl.ds(pl.multiple_of(2 * z, 2), 2) if pooled else me
        copies = slab_copies(step, slot)
        groups = [(0,), (1,)] if step == 0 else [(0, 1)]
        for group in groups:
            for half in group:
                copies[half].wait()
                if step == 0:
                    fetch(2, half)
            made = _dot(a_s[tokens, :], slab_s[slot, :, group[0] * (SLAB // 2) : (group[-1] + 1) * (SLAB // 2)], 1, 0)
            if group[-1]:
                for k in range(2):
                    fetch(step + SLABS, k)
            for half in group:
                for i in range(2):
                    t = made[:, ((half - group[0]) * 2 + i) * HEAD :][:, :HEAD]
                    t = t.T.astype(bf16) if half else turned(t, cos_ref[tokens, :], sin_ref[tokens, :])
                    if other:
                        stage_s[i, half] = t
                    elif pooled:
                        for j in range(2):
                            part_of = slice(j * own, (j + 1) * own)
                            kv_s[2 * p + i, half, 2 * z + j] = t[:, part_of] if half else t[part_of, :]
                    else:
                        kv_s[2 * p + i, half, me] = t
                dst = kv_s.at[pl.ds(2 * p, 2), half, block]
                src = stage_s.at[:, half] if other else dst
                at = 2 * step + half
                sends = [(wanted(0, 1, right), remote(src, dst, s1_send.at[at, 0], s1_recv.at[0, at], right * 2 + core)),
                         (wanted(1, 1, left), remote(src, dst, s1_send.at[at, 1], s1_recv.at[1, at], left * 2 + core))]
                if other:
                    sends.append((True, remote(src, dst, s1_send.at[at, 2], sp_recv.at[half], partner)))
                for needed, copy in sends:
                    pl.when(needed)(copy.start)
                first_sends += sends
        if step == 0:
            x_send.wait_send()
            remote(x_s.at[theirs, :], x_s.at[theirs, :], xs_send, xs_recv, partner).wait_recv()
            norm_rows((1 - c) * own)

    def part(d, s, h, at):
        blocks = pl.ds(pl.multiple_of(2 * at, 2), 2)
        return kv_s.at[h, :, blocks] if s < nz // 2 else kv_s.at[h, d, blocks]

    def passing(d, s, h):
        at = chunk_at(-(s - 1) if d == 0 else s - 1)
        ref = part(d, s, h, at)
        return remote(ref, ref, f_send.at[d, s - 2, h], f_recv.at[d, s - 2, h], (right if d == 0 else left) * 2 + c)

    def coming(d, s, h):
        ref = part(d, s, h, chunk_at(-s if d == 0 else s))
        return remote(ref, ref, f_send.at[d, s - 2, h], f_recv.at[d, s - 2, h], partner)

    def first_arrived(p):
        for d in range(2):
            @pl.when(wanted(d, 1, z))
            def _():
                at = chunk_at(-1 if d == 0 else 1)
                if p == 0:
                    whose = [(0, at * 2 + c), (1, at * 2 + 1 - c)]
                else:
                    whose = [(p + 1, pl.ds(pl.multiple_of(2 * at, 2), 2))]
                for step, block in whose:
                    for half in range(2):
                        ref = kv_s.at[pl.ds(2 * p, 2), half, block]
                        remote(ref, ref, xs_send, s1_recv.at[d, 2 * step + half], partner).wait_recv()

    def arrived(s, h):
        for d in range(2):
            pl.when(wanted(d, s, z))(coming(d, s, h).wait_recv)

    def forward(s, h):
        for d in range(2):
            pl.when(wanted(d, s, right if d == 0 else left))(passing(d, s, h).start)

    def turn_queries(i):
        for k in range(SLAB // HEAD):
            at = pl.multiple_of((i * (SLAB // HEAD) + k) * both, both)
            q_s[pl.ds(at, both), :] = turned(made_s[:, k * HEAD : (k + 1) * HEAD], cos_ref[...], sin_ref[...])

    made_s[...] = jnp.zeros((both, SLAB), f32)

    def q_step(i, _):
        slot = lax.rem(i + kv_steps, SLABS)
        for copy in q_copies(i, slot):
            copy.wait()
        turn_queries(jnp.maximum(i - 1, 0))
        made_s[...] = _dot(a_s[...], slab_s[slot], 1, 0)
        at = pl.ds(pl.multiple_of(i * SLAB, SLAB), SLAB)
        acc_s[:, at] = x_s[:, pl.ds(pl.multiple_of(c * yw + i * SLAB, SLAB), SLAB)].astype(f32)

        @pl.when(i < qw // SLAB - SLABS)
        def _():
            for copy in q_copies(i + SLABS, slot):
                copy.start()

        @pl.when(i == 1)
        def _():
            first_arrived(0)
            forward(2, 0)
            forward(2, 1)

        @pl.when(i == 4)
        def _():
            first_arrived(1)
            forward(2, 2)

    lax.fori_loop(0, qw // SLAB, q_step, None)
    pl.semaphore_signal(ready, inc=1, device_id={"sp": partner}, device_id_type=pl.DeviceIdType.MESH)
    turn_queries(qw // SLAB - 1)
    for grp in range(2):
        for k in range(2):
            for copy in wo_copies(grp, k):
                copy.start()
    for half in range(2):
        ref = kv_s.at[pl.ds(0, 2), half, partner]
        remote(ref, ref, xs_send, sp_recv.at[half], partner).wait_recv()

    def attend(p, heads, chunks, own_chunk=False):
        strips = [(nth, at) for nth in range(len(heads)) for at in range(0, cols, WIDE)]
        loaded = {}
        if own_chunk:
            shape = (both, WIDE)
            ok = lax.broadcasted_iota(jnp.int32, shape, 0) <= lax.rem(lax.broadcasted_iota(jnp.int32, shape, 1), both)

        def keys_of(nth):
            if nth not in loaded:
                h = 2 * p + heads[nth]
                keys = jnp.concatenate([kv_s[h, 0, pl.ds(2 * b, 2)].reshape(both, HEAD) for b in chunks], axis=0)
                values = jnp.concatenate([kv_s[h, 1, 2 * b + j] for b in chunks for j in range(2)], axis=1)
                loaded[nth] = keys, jnp.concatenate([values, jnp.ones((8, values.shape[1]), bf16)], axis=0)
            return loaded[nth]

        def score(nth, at):
            return _dot(keys_of(nth)[0], q_s[pl.ds(pl.multiple_of((2 * p + heads[nth]) * cols + at, WIDE), WIDE), :], 1, 1) * e

        scores = [score(*strip) for strip in strips[:AHEAD]]
        for m, (nth, at) in enumerate(strips):
            i = heads[nth]
            if m + AHEAD < len(strips):
                scores.append(score(*strips[m + AHEAD]))
            s, here = scores[m], slice(at, at + WIDE)
            if own_chunk:
                s = jnp.where(ok, s, HIDDEN)
                top = s.max(axis=0, keepdims=True)
            else:
                old = top_s[p, i, :, here]
                top = jnp.maximum(old, s.max(axis=0, keepdims=True))
            top_s[p, i, :, here] = top
            add = _dot(keys_of(nth)[1], jnp.exp2(s - top).astype(bf16), 1, 0)
            mix_s[p, i, :, here] = add if own_chunk else mix_s[p, i, :, here] * jnp.exp2(old - top) + add

    def attend_at(p, s, heads=(0, 1)):
        before, after = z >= s, z + s >= nz
        lower, upper = chunk_at(-s), chunk_at(s)

        @pl.when(before & after)
        def _():
            attend(p, heads, [lower, upper])

        @pl.when(before != after)
        def _():
            attend(p, heads, [jnp.where(before, lower, upper)])

    def seen(whose, h):
        return x_s.at[:, pl.ds(pl.multiple_of(whose * qw + h * gw, gw), gw)]

    def seen_copy(h):
        return remote(seen(c, h), seen(c, h), seen_send.at[h], seen_recv.at[h], partner)

    def seen_arrived(h):
        remote(seen(1 - c, h), seen(1 - c, h), seen_send.at[h], seen_recv.at[h], partner).wait_recv()

    def product(grp, k, at):
        return _dot(seen(1 - c if k else c, grp)[...], wo_s[grp % 2, k, :, at], 1, 0)

    def blocks(body, width=OUTW):
        def block(i, _):
            body(i, pl.ds(pl.multiple_of(i * width, width), width))

        lax.fori_loop(0, yw // width, block, None)

    def project(grp, parts=(0, 1)):
        for k in parts:
            for copy in wo_copies(grp, k):
                copy.wait()
        if 1 in parts:
            seen_arrived(grp)

        def body(_, at):
            acc_s[:, at] = acc_s[:, at] + sum(product(grp, k, at) for k in parts)

        blocks(body)
        if 1 in parts and grp + 2 < hk:
            for k in range(2):
                for copy in wo_copies(grp + 2, k):
                    copy.start()

    def out_copy(i):
        at = pl.ds(pl.multiple_of(i * LASTW, LASTW), LASTW)
        to = pl.ds(pl.multiple_of(c * yw + i * LASTW, LASTW), LASTW)
        return remote(a_s.at[theirs, at], out_ref.at[:, to], y_send.at[i], y_recv.at[i], partner)

    def finish(h, p, i):
        arrived(nz // 2, h)

        @pl.when(z >= nz // 2)
        def _():
            attend(p, (i,), [chunk_at(nz // 2)])

        inverse = 1 / mix_s[p, i, HEAD : HEAD + 1, :]
        for k in range(g):
            at = slice(k * both, (k + 1) * both)
            seen(c, h)[:, k * HEAD : (k + 1) * HEAD] = (mix_s[p, i, :HEAD, at] * inverse[:, at]).T.astype(bf16)
        seen_copy(h).start()

    order = [(0, 0), (0, 1), (1, 0), (1, 1), (0, 2), (0, 3), (1, 2), (1, 3)]

    def pick(k, values):
        at = jnp.int32(values[-1])
        for n_, value in enumerate(values[:-1]):
            at = jnp.where(k == n_, value, at)
        return at

    def stage(k, _):
        p, s = pick(k, [a for a, _ in order]), pick(k, [b for _, b in order])

        @pl.when(s == 0)
        def _():
            attend(p, (0, 1), [z], own_chunk=True)

        @pl.when((s > 0) & (k != 5))
        def _():
            attend_at(p, s)

        @pl.when(k == 0)
        def _():
            arrived(2, 0)
            forward(3, 0)

        @pl.when(k == 1)
        def _():
            arrived(2, 1)
            forward(3, 1)

        @pl.when(k == 4)
        def _():
            arrived(3, 0)
            forward(4, 0)
            forward(2, 3)

        @pl.when(k == 5)
        def _():
            def head(i, _):
                @pl.when(i == 1)
                def _():
                    arrived(3, 1)
                    forward(4, 1)

                attend_at(0, 3, (i,))

            lax.fori_loop(0, 2, head, None)
            arrived(2, 2)
            forward(3, 2)
            pl.semaphore_wait(ready, 1)
            finish(0, 0, 0)
            project(0, (0,))
            arrived(2, 3)
            forward(3, 3)

        @pl.when(k == 6)
        def _():
            finish(1, 0, 1)
            arrived(3, 2)
            forward(4, 2)
            project(0, (1,))
            project(1)
            arrived(3, 3)
            forward(4, 3)

    lax.fori_loop(0, len(order), stage, None)
    finish(2, 1, 0)
    project(2, (0,))
    finish(3, 1, 1)
    project(2, (1,))

    last = hk - 1
    for k in range(2):
        for copy in wo_copies(last, k):
            copy.wait()
    seen_arrived(last)

    def final(i, at):
        a_s[:, at] = (acc_s[:, at] + (product(last, 0, at) + product(last, 1, at))).astype(bf16)
        out_copy(i).start()
        out_ref[:, pl.ds(pl.multiple_of(c * yw + i * LASTW, LASTW), LASTW)] = a_s[mine, at]

    blocks(final, LASTW)

    for needed, copy in first_sends:
        pl.when(needed)(copy.wait_send)
    for s in range(2, nz // 2 + 1):
        for d in range(2):
            @pl.when(wanted(d, s, right if d == 0 else left))
            def _():
                for h in range(hk):
                    passing(d, s, h).wait_send()
    for h in range(hk):
        seen_copy(h).wait_send()
    for i in range(yw // LASTW):
        out_copy(i).wait_send()
        to = pl.ds(pl.multiple_of((1 - c) * yw + i * LASTW, LASTW), LASTW)
        remote(out_ref.at[:, to], out_ref.at[:, to], y_send.at[i], y_recv.at[i], partner).wait_recv()


def solution(mesh):
    n = mesh.shape["sp"]

    def step(x, gain, wq, wk, wv, wo):
        own, dim = x.shape
        both = 2 * own
        hk = wk.shape[1] // HEAD // 2
        qw = wq.shape[1] // 2
        g = qw // HEAD // hk
        cols = g * both
        vmem, hbm = pl.BlockSpec(memory_space=pltpu.VMEM), pl.BlockSpec(memory_space=pl.ANY)
        dma = pltpu.SemaphoreType.DMA
        blocks = dim // 2 // LASTW
        return pl.pallas_call(
            functools.partial(_kernel, n),
            out_shape=pltpu.VMEM((own, dim), bf16),
            in_specs=[hbm, vmem, hbm, hbm, hbm, hbm],
            out_specs=vmem,
            scratch_shapes=[
                pltpu.VMEM((ROWS, dim), f32),
                pltpu.VMEM((both, HEAD), f32),
                pltpu.VMEM((both, HEAD), f32),
                pltpu.VMEM((both, dim), bf16),
                pltpu.VMEM((both, dim), bf16),
                pltpu.VMEM((hk * g * both, HEAD), bf16),
                pltpu.VMEM((hk, 2, n, own, HEAD), bf16),
                pltpu.VMEM((2, 2, own, HEAD), bf16),
                pltpu.VMEM((both, SLAB), f32),
                pltpu.VMEM((hk // 2, 2, 1, cols), f32),
                pltpu.VMEM((hk // 2, 2, HEAD + 8, cols), f32),
                pltpu.VMEM((both, dim // 2), f32),
                pltpu.VMEM((SLABS, dim, SLAB), bf16),
                pltpu.VMEM((2, 2, g * HEAD, dim // 2), bf16),
                dma, dma((SLABS, 2)), dma((2, 2, 2)), dma, dma, dma((hk + 2, 3)), dma((2, hk + 2)), dma((2,)),
                dma((2, 3, hk)), dma((2, 3, hk)), dma((hk,)), dma((hk,)), dma((blocks,)), dma((blocks,)), pltpu.SemaphoreType.REGULAR,
            ],
            compiler_params=pltpu.CompilerParams(collective_id=0, has_side_effects=True, vmem_limit_bytes=VMEM),
        )(x, gain.reshape(dim // HEAD, HEAD), wq, wk, wv, wo)

    tokens, whole = P(("dp", "sp"), None), P(None, None)
    return jax.shard_map(
        step,
        mesh=mesh,
        in_specs=(tokens, P(None), whole, whole, whole, whole),
        out_specs=tokens,
        check_vma=False,
    )
```

```python
import functools
import math

import jax
import jax.numpy as jnp
from jax import lax
from jax.experimental import pallas as pl
from jax.experimental.pallas import tpu as pltpu
from jax.sharding import PartitionSpec as P

HEAD = 128
THETA = 10000
HIDDEN = -2e30
LOG2E = 1.4426950408889634
VMEM = 62 * 2**20
SLAB = 512
WIDE = 256
AHEAD = 3
OUTW = 1536
LASTW = 1024
SLABS = 3
ROWS = 16

bf16, f32 = jnp.bfloat16, jnp.float32


def _dot(a, b, ca, cb):
    return lax.dot_general(a, b, (((ca,), (cb,)), ((), ())), preferred_element_type=f32)


def _kernel(n, x_hbm, gain_ref, wq, wk, wv, wo, out_ref, gain_s, cos_ref, sin_ref, x_s, a_s, q_s, kv_s, stage_s, made_s, top_s, mix_s, acc_s, slab_s, wo_s,
            x_sem, slab_sem, wo_sem, xs_send, xs_recv, s1_send, s1_recv, sp_recv, f_send, f_recv,
            seen_send, seen_recv, y_send, y_recv, ready):
    me = lax.axis_index("sp")
    c, z = lax.rem(me, 2), lax.div(me, 2)
    nz = n // 2
    partner = me + 1 - 2 * c
    left, right = lax.rem(z + nz - 1, nz), lax.rem(z + 1, nz)
    own, dim = x_hbm.shape
    both = 2 * own
    hk = kv_s.shape[0]
    g = q_s.shape[0] // (both * hk)
    cols = g * both
    kvw, qw = wk.shape[1] // 2, wq.shape[1] // 2
    yw = dim // 2
    pairs = hk // 2
    kv_steps = pairs + 1
    gw = g * HEAD
    e = HEAD**-0.5 * LOG2E

    def chunk_at(offset):
        return lax.rem(z + offset + 2 * nz, nz)

    def wanted(d, s, to):
        return to >= s if d == 0 else (to + s >= nz) | (to + s < nz // 2)

    def remote(src, dst, send, recv, to):
        return pltpu.make_async_remote_copy(src_ref=src, dst_ref=dst, send_sem=send, recv_sem=recv, device_id={"sp": to},
                                            device_id_type=pl.DeviceIdType.MESH)

    def slab_copies(step, slot):
        at = pl.multiple_of((1 - c if step == 1 else c) * kvw + max(step - 1, 0) * 2 * HEAD, 2 * HEAD)
        return [pltpu.make_async_copy(w.at[:, pl.ds(at, SLAB // 2)], slab_s.at[slot, :, pl.ds(i * (SLAB // 2), SLAB // 2)],
                                      slab_sem.at[slot, i]) for i, w in enumerate((wk, wv))]

    def q_copies(i, slot):
        return [pltpu.make_async_copy(wq.at[:, pl.ds(pl.multiple_of(c * qw + i * SLAB + k * (SLAB // 2), SLAB // 2), SLAB // 2)],
                                      slab_s.at[slot, :, pl.ds(k * (SLAB // 2), SLAB // 2)], slab_sem.at[slot, k]) for k in range(2)]

    def wo_copies(grp, k):
        row = (1 - c if k else c) * qw + grp * gw
        half = gw // 2
        return [pltpu.make_async_copy(wo.at[pl.ds(pl.multiple_of(row + i * half, half), half), pl.ds(pl.multiple_of(c * yw, yw), yw)],
                                      wo_s.at[grp % 2, k, pl.ds(i * half, half), :], wo_sem.at[grp % 2, k, i])
                for i in range(2)]

    mine = pl.ds(pl.multiple_of(c * own, own), own)
    theirs = pl.ds(pl.multiple_of((1 - c) * own, own), own)
    def fetch(step, k):
        (slab_copies(step, step % SLABS) if step < kv_steps else q_copies(step - kv_steps, step % SLABS))[k].start()

    x_copy = pltpu.make_async_copy(x_hbm, x_s.at[mine, :], x_sem)
    x_copy.start()
    fetch(0, 0)

    barrier = pltpu.get_barrier_semaphore()
    near = [partner, left * 2 + c, right * 2 + c, left * 2 + 1 - c, right * 2 + 1 - c]
    for to in near:
        pl.semaphore_signal(barrier, inc=1, device_id={"sp": to}, device_id_type=pl.DeviceIdType.MESH)

    for i in range(dim // HEAD):
        gain_s[:, i * HEAD : (i + 1) * HEAD] = jnp.broadcast_to(gain_ref[i : i + 1, :].astype(f32), (ROWS, HEAD))
    element = lax.broadcasted_iota(jnp.int32, (both, HEAD), 1)
    half = HEAD // 2
    power = jnp.where(element < half, element, element - half).astype(f32)
    place = (z * both + lax.broadcasted_iota(jnp.int32, (both, HEAD), 0)).astype(f32)
    angle = place * jnp.exp2(power * (-math.log2(THETA) / half))
    cos_ref[...] = jnp.cos(angle)
    sine = jnp.sin(angle)
    sin_ref[...] = jnp.where(element < half, -sine, sine)

    x_copy.wait()
    for step, k in ((0, 1), (1, 0), (1, 1)):
        fetch(step, k)

    def norm_rows(start):
        def rows(i, _):
            for k in range(2):
                r = pl.ds(pl.multiple_of(start + (2 * i + k) * ROWS, ROWS), ROWS)
                wide = x_s[r, :].astype(f32)
                scale = lax.rsqrt(jnp.mean(wide * wide, -1, keepdims=True) + 1e-6)
                a_s[r, :] = (wide * scale * gain_s[...]).astype(bf16)

        lax.fori_loop(0, own // ROWS // 2, rows, None)

    pl.semaphore_wait(barrier, len(near))
    x_send = remote(x_s.at[mine, :], x_s.at[mine, :], xs_send, xs_recv, partner)
    x_send.start()
    norm_rows(c * own)

    def turned(t, cos, sin):
        t = t.astype(bf16).astype(f32)
        return (t * cos + pltpu.roll(t, HEAD // 2, 1) * sin).astype(bf16)

    first_sends = []
    for step in range(kv_steps):
        slot, p, other = step % SLABS, max(step - 1, 0), step == 1
        pooled = step > 1
        tokens = slice(None) if pooled else mine
        core = 1 - c if other else c
        block = pl.ds(pl.multiple_of(2 * z, 2), 2) if pooled else me
        copies = slab_copies(step, slot)
        groups = [(0,), (1,)] if step == 0 else [(0, 1)]
        for group in groups:
            for half in group:
                copies[half].wait()
                if step == 0:
                    fetch(2, half)
            made = _dot(a_s[tokens, :], slab_s[slot, :, group[0] * (SLAB // 2) : (group[-1] + 1) * (SLAB // 2)], 1, 0)
            if group[-1]:
                for k in range(2):
                    fetch(step + SLABS, k)
            for half in group:
                for i in range(2):
                    t = made[:, ((half - group[0]) * 2 + i) * HEAD :][:, :HEAD]
                    t = t.T.astype(bf16) if half else turned(t, cos_ref[tokens, :], sin_ref[tokens, :])
                    if other:
                        stage_s[i, half] = t
                    elif pooled:
                        for j in range(2):
                            part_of = slice(j * own, (j + 1) * own)
                            kv_s[2 * p + i, half, 2 * z + j] = t[:, part_of] if half else t[part_of, :]
                    else:
                        kv_s[2 * p + i, half, me] = t
                dst = kv_s.at[pl.ds(2 * p, 2), half, block]
                src = stage_s.at[:, half] if other else dst
                at = 2 * step + half
                sends = [(wanted(0, 1, right), remote(src, dst, s1_send.at[at, 0], s1_recv.at[0, at], right * 2 + core)),
                         (wanted(1, 1, left), remote(src, dst, s1_send.at[at, 1], s1_recv.at[1, at], left * 2 + core))]
                if other:
                    sends.append((True, remote(src, dst, s1_send.at[at, 2], sp_recv.at[half], partner)))
                for needed, copy in sends:
                    pl.when(needed)(copy.start)
                first_sends += sends
        if step == 0:
            x_send.wait_send()
            remote(x_s.at[theirs, :], x_s.at[theirs, :], xs_send, xs_recv, partner).wait_recv()
            norm_rows((1 - c) * own)

    def part(d, s, h, at):
        blocks = pl.ds(pl.multiple_of(2 * at, 2), 2)
        return kv_s.at[h, :, blocks] if s < nz // 2 else kv_s.at[h, d, blocks]

    def passing(d, s, h):
        at = chunk_at(-(s - 1) if d == 0 else s - 1)
        ref = part(d, s, h, at)
        return remote(ref, ref, f_send.at[d, s - 2, h], f_recv.at[d, s - 2, h], (right if d == 0 else left) * 2 + c)

    def coming(d, s, h):
        ref = part(d, s, h, chunk_at(-s if d == 0 else s))
        return remote(ref, ref, f_send.at[d, s - 2, h], f_recv.at[d, s - 2, h], partner)

    def first_arrived(p):
        for d in range(2):
            @pl.when(wanted(d, 1, z))
            def _():
                at = chunk_at(-1 if d == 0 else 1)
                if p == 0:
                    whose = [(0, at * 2 + c), (1, at * 2 + 1 - c)]
                else:
                    whose = [(p + 1, pl.ds(pl.multiple_of(2 * at, 2), 2))]
                for step, block in whose:
                    for half in range(2):
                        ref = kv_s.at[pl.ds(2 * p, 2), half, block]
                        remote(ref, ref, xs_send, s1_recv.at[d, 2 * step + half], partner).wait_recv()

    def arrived(s, h):
        for d in range(2):
            pl.when(wanted(d, s, z))(coming(d, s, h).wait_recv)

    def forward(s, h):
        for d in range(2):
            pl.when(wanted(d, s, right if d == 0 else left))(passing(d, s, h).start)

    def turn_queries(i):
        for k in range(SLAB // HEAD):
            at = pl.multiple_of((i * (SLAB // HEAD) + k) * both, both)
            q_s[pl.ds(at, both), :] = turned(made_s[:, k * HEAD : (k + 1) * HEAD], cos_ref[...], sin_ref[...])

    made_s[...] = jnp.zeros((both, SLAB), f32)

    def q_step(i, _):
        slot = lax.rem(i + kv_steps, SLABS)
        for copy in q_copies(i, slot):
            copy.wait()
        turn_queries(jnp.maximum(i - 1, 0))
        made_s[...] = _dot(a_s[...], slab_s[slot], 1, 0)
        at = pl.ds(pl.multiple_of(i * SLAB, SLAB), SLAB)
        acc_s[:, at] = x_s[:, pl.ds(pl.multiple_of(c * yw + i * SLAB, SLAB), SLAB)].astype(f32)

        @pl.when(i < qw // SLAB - SLABS)
        def _():
            for copy in q_copies(i + SLABS, slot):
                copy.start()

        @pl.when(i == 1)
        def _():
            first_arrived(0)
            forward(2, 0)
            forward(2, 1)

        @pl.when(i == 4)
        def _():
            first_arrived(1)
            forward(2, 2)

    lax.fori_loop(0, qw // SLAB, q_step, None)
    pl.semaphore_signal(ready, inc=1, device_id={"sp": partner}, device_id_type=pl.DeviceIdType.MESH)
    turn_queries(qw // SLAB - 1)
    for grp in range(2):
        for k in range(2):
            for copy in wo_copies(grp, k):
                copy.start()
    for half in range(2):
        ref = kv_s.at[pl.ds(0, 2), half, partner]
        remote(ref, ref, xs_send, sp_recv.at[half], partner).wait_recv()

    def attend(p, heads, chunks, own_chunk=False):
        strips = [(nth, at) for nth in range(len(heads)) for at in range(0, cols, WIDE)]
        loaded = {}
        if own_chunk:
            shape = (both, WIDE)
            ok = lax.broadcasted_iota(jnp.int32, shape, 0) <= lax.rem(lax.broadcasted_iota(jnp.int32, shape, 1), both)

        def keys_of(nth):
            if nth not in loaded:
                h = 2 * p + heads[nth]
                keys = jnp.concatenate([kv_s[h, 0, pl.ds(2 * b, 2)].reshape(both, HEAD) for b in chunks], axis=0)
                values = jnp.concatenate([kv_s[h, 1, 2 * b + j] for b in chunks for j in range(2)], axis=1)
                loaded[nth] = keys, jnp.concatenate([values, jnp.ones((8, values.shape[1]), bf16)], axis=0)
            return loaded[nth]

        def score(nth, at):
            return _dot(keys_of(nth)[0], q_s[pl.ds(pl.multiple_of((2 * p + heads[nth]) * cols + at, WIDE), WIDE), :], 1, 1) * e

        scores = [score(*strip) for strip in strips[:AHEAD]]
        for m, (nth, at) in enumerate(strips):
            i = heads[nth]
            if m + AHEAD < len(strips):
                scores.append(score(*strips[m + AHEAD]))
            s, here = scores[m], slice(at, at + WIDE)
            if own_chunk:
                s = jnp.where(ok, s, HIDDEN)
                top = s.max(axis=0, keepdims=True)
            else:
                old = top_s[p, i, :, here]
                top = jnp.maximum(old, s.max(axis=0, keepdims=True))
            top_s[p, i, :, here] = top
            add = _dot(keys_of(nth)[1], jnp.exp2(s - top).astype(bf16), 1, 0)
            mix_s[p, i, :, here] = add if own_chunk else mix_s[p, i, :, here] * jnp.exp2(old - top) + add

    def attend_at(p, s, heads=(0, 1)):
        before, after = z >= s, z + s >= nz
        lower, upper = chunk_at(-s), chunk_at(s)

        @pl.when(before & after)
        def _():
            attend(p, heads, [lower, upper])

        @pl.when(before != after)
        def _():
            attend(p, heads, [jnp.where(before, lower, upper)])

    def seen(whose, h):
        return x_s.at[:, pl.ds(pl.multiple_of(whose * qw + h * gw, gw), gw)]

    def seen_copy(h):
        return remote(seen(c, h), seen(c, h), seen_send.at[h], seen_recv.at[h], partner)

    def seen_arrived(h):
        remote(seen(1 - c, h), seen(1 - c, h), seen_send.at[h], seen_recv.at[h], partner).wait_recv()

    def product(grp, k, at):
        return _dot(seen(1 - c if k else c, grp)[...], wo_s[grp % 2, k, :, at], 1, 0)

    def blocks(body, width=OUTW):
        def block(i, _):
            body(i, pl.ds(pl.multiple_of(i * width, width), width))

        lax.fori_loop(0, yw // width, block, None)

    def project(grp, parts=(0, 1)):
        for k in parts:
            for copy in wo_copies(grp, k):
                copy.wait()
        if 1 in parts:
            seen_arrived(grp)

        def body(_, at):
            acc_s[:, at] = acc_s[:, at] + sum(product(grp, k, at) for k in parts)

        blocks(body)
        if 1 in parts and grp + 2 < hk:
            for k in range(2):
                for copy in wo_copies(grp + 2, k):
                    copy.start()

    def out_copy(i):
        at = pl.ds(pl.multiple_of(i * LASTW, LASTW), LASTW)
        to = pl.ds(pl.multiple_of(c * yw + i * LASTW, LASTW), LASTW)
        return remote(a_s.at[theirs, at], out_ref.at[:, to], y_send.at[i], y_recv.at[i], partner)

    def finish(h, p, i):
        arrived(nz // 2, h)

        @pl.when(z >= nz // 2)
        def _():
            attend(p, (i,), [chunk_at(nz // 2)])

        inverse = 1 / mix_s[p, i, HEAD : HEAD + 1, :]
        for k in range(g):
            at = slice(k * both, (k + 1) * both)
            seen(c, h)[:, k * HEAD : (k + 1) * HEAD] = (mix_s[p, i, :HEAD, at] * inverse[:, at]).T.astype(bf16)
        seen_copy(h).start()

    order = [(0, 0), (0, 1), (1, 0), (1, 1), (0, 2), (0, 3), (1, 2), (1, 3)]

    def pick(k, values):
        at = jnp.int32(values[-1])
        for n_, value in enumerate(values[:-1]):
            at = jnp.where(k == n_, value, at)
        return at

    def stage(k, _):
        p, s = pick(k, [a for a, _ in order]), pick(k, [b for _, b in order])

        @pl.when(s == 0)
        def _():
            attend(p, (0, 1), [z], own_chunk=True)

        @pl.when((s > 0) & (k != 5))
        def _():
            attend_at(p, s)

        @pl.when(k == 0)
        def _():
            arrived(2, 0)
            forward(3, 0)

        @pl.when(k == 1)
        def _():
            arrived(2, 1)
            forward(3, 1)

        @pl.when(k == 4)
        def _():
            arrived(3, 0)
            forward(4, 0)
            forward(2, 3)

        @pl.when(k == 5)
        def _():
            def head(i, _):
                @pl.when(i == 1)
                def _():
                    arrived(3, 1)
                    forward(4, 1)

                attend_at(0, 3, (i,))

            lax.fori_loop(0, 2, head, None)
            arrived(2, 2)
            forward(3, 2)
            pl.semaphore_wait(ready, 1)
            finish(0, 0, 0)
            project(0, (0,))
            arrived(2, 3)
            forward(3, 3)

        @pl.when(k == 6)
        def _():
            finish(1, 0, 1)
            project(0, (1,))
            arrived(3, 2)
            forward(4, 2)
            project(1)
            arrived(3, 3)
            forward(4, 3)

    lax.fori_loop(0, len(order), stage, None)
    finish(2, 1, 0)
    project(2, (0,))
    finish(3, 1, 1)
    project(2, (1,))

    last = hk - 1
    for k in range(2):
        for copy in wo_copies(last, k):
            copy.wait()
    seen_arrived(last)

    def final(i, at):
        a_s[:, at] = (acc_s[:, at] + (product(last, 0, at) + product(last, 1, at))).astype(bf16)
        out_copy(i).start()
        out_ref[:, pl.ds(pl.multiple_of(c * yw + i * LASTW, LASTW), LASTW)] = a_s[mine, at]

    blocks(final, LASTW)

    for needed, copy in first_sends:
        pl.when(needed)(copy.wait_send)
    for s in range(2, nz // 2 + 1):
        for d in range(2):
            @pl.when(wanted(d, s, right if d == 0 else left))
            def _():
                for h in range(hk):
                    passing(d, s, h).wait_send()
    for h in range(hk):
        seen_copy(h).wait_send()
    for i in range(yw // LASTW):
        out_copy(i).wait_send()
        to = pl.ds(pl.multiple_of((1 - c) * yw + i * LASTW, LASTW), LASTW)
        remote(out_ref.at[:, to], out_ref.at[:, to], y_send.at[i], y_recv.at[i], partner).wait_recv()


def solution(mesh):
    n = mesh.shape["sp"]

    def step(x, gain, wq, wk, wv, wo):
        own, dim = x.shape
        both = 2 * own
        hk = wk.shape[1] // HEAD // 2
        qw = wq.shape[1] // 2
        g = qw // HEAD // hk
        cols = g * both
        vmem, hbm = pl.BlockSpec(memory_space=pltpu.VMEM), pl.BlockSpec(memory_space=pl.ANY)
        dma = pltpu.SemaphoreType.DMA
        blocks = dim // 2 // LASTW
        return pl.pallas_call(
            functools.partial(_kernel, n),
            out_shape=pltpu.VMEM((own, dim), bf16),
            in_specs=[hbm, vmem, hbm, hbm, hbm, hbm],
            out_specs=vmem,
            scratch_shapes=[
                pltpu.VMEM((ROWS, dim), f32),
                pltpu.VMEM((both, HEAD), f32),
                pltpu.VMEM((both, HEAD), f32),
                pltpu.VMEM((both, dim), bf16),
                pltpu.VMEM((both, dim), bf16),
                pltpu.VMEM((hk * g * both, HEAD), bf16),
                pltpu.VMEM((hk, 2, n, own, HEAD), bf16),
                pltpu.VMEM((2, 2, own, HEAD), bf16),
                pltpu.VMEM((both, SLAB), f32),
                pltpu.VMEM((hk // 2, 2, 1, cols), f32),
                pltpu.VMEM((hk // 2, 2, HEAD + 8, cols), f32),
                pltpu.VMEM((both, dim // 2), f32),
                pltpu.VMEM((SLABS, dim, SLAB), bf16),
                pltpu.VMEM((2, 2, g * HEAD, dim // 2), bf16),
                dma, dma((SLABS, 2)), dma((2, 2, 2)), dma, dma, dma((hk + 2, 3)), dma((2, hk + 2)), dma((2,)),
                dma((2, 3, hk)), dma((2, 3, hk)), dma((hk,)), dma((hk,)), dma((blocks,)), dma((blocks,)), pltpu.SemaphoreType.REGULAR,
            ],
            compiler_params=pltpu.CompilerParams(collective_id=0, has_side_effects=True, vmem_limit_bytes=VMEM),
        )(x, gain.reshape(dim // HEAD, HEAD), wq, wk, wv, wo)

    tokens, whole = P(("dp", "sp"), None), P(None, None)
    return jax.shard_map(
        step,
        mesh=mesh,
        in_specs=(tokens, P(None), whole, whole, whole, whole),
        out_specs=tokens,
        check_vma=False,
    )
```
